16 devices in a mesh: dp: 2 (over y, z), dcp: 8 (over x, core).
Axes of the slice: x: 4, y: 2, z: 1, core: 2. Of those that a mesh axis runs over, the one named last changes fastest.
The devices are a block of a 4x4x8 slice.
Arguments:
- q_abs: bfloat16 [128, 128, 576], P('dp', 'dcp'), parts along dimension 0
- latent_cache: bfloat16 [128, 4, 8, 256, 576], P('dp', None, 'dcp'), parts along dimension 0
- ctx_len: int32 [128], P('dp'), parts along dimension 0
Outputs:
- output: bfloat16 [128, 128, 512], P(('dp', 'dcp')), parts along dimension 0
There are 2 independent parts. The reference program is written for one: setup_inputs(seed, part) draws one part's arguments, and reference() takes and returns one part's arrays. A program takes and returns all parts, laid end to end along the dimension named above; each array names one.
All inputs are finite; a program needn't handle non-finite values.
Results may differ from the reference program's by a relative error of at most 0.00644916.
Values are sent between devices in bfloat16 or wider.
A program may use at most 768 MiB of HBM per device.

```python
import math
import jax
import jax.numpy as jnp
from jax import lax

BATCH_SIZE = 64
NUM_HEADS = 128
LATENT_DIM = 512
ROPE_DIM = 64
NOPE_DIM = 128
PAGES_DEV = 4
GROUP_SIZE = 8
PAGE_LEN = 256

WIDTH = LATENT_DIM + ROPE_DIM
SEQ_LEN = PAGES_DEV * GROUP_SIZE * PAGE_LEN


def setup_inputs(seed: int = 0, part: int = 0) -> dict:
    part_key = jax.random.fold_in(jax.random.key(seed), part)
    key_query, key_cache, key_len = jax.random.split(part_key, 3)
    qk_dim = NOPE_DIM + ROPE_DIM
    cache_rope = 1.4
    query_latent = math.sqrt(0.95 * qk_dim / LATENT_DIM)
    query_rope = math.sqrt(0.95 * qk_dim / ROPE_DIM) / cache_rope
    is_latent = jnp.arange(WIDTH) < LATENT_DIM
    query_scale = jnp.where(is_latent, query_latent, query_rope)
    cache_scale = jnp.where(is_latent, 1.0, cache_rope)
    queries = jax.random.normal(key_query, (BATCH_SIZE, NUM_HEADS, WIDTH), jnp.float32) * query_scale
    cache_vals = jax.random.normal(key_cache, (BATCH_SIZE, PAGES_DEV, GROUP_SIZE, PAGE_LEN, WIDTH), jnp.float32) * cache_scale
    len_drop = jax.random.randint(key_len, (BATCH_SIZE,), 0, SEQ_LEN // 2)
    lengths = jnp.where(jnp.arange(BATCH_SIZE) == 0, SEQ_LEN, SEQ_LEN - len_drop)
    return {'q_abs': queries.astype(jnp.bfloat16), 'latent_cache': cache_vals.astype(jnp.bfloat16), 'ctx_len': lengths.astype(jnp.int32)}


def reference(q_abs, latent_cache, ctx_len):
    inv_scale = (NOPE_DIM + ROPE_DIM) ** -0.5
    q_float = q_abs.astype(jnp.float32)
    per_device = jnp.moveaxis(latent_cache, 2, 0)
    page_base = jnp.arange(PAGES_DEV)[:, None] * (GROUP_SIZE * PAGE_LEN) + jnp.arange(PAGE_LEN)[None, :]

    def one_device(carry_in):
        dev_index, cache_blk = carry_in
        cache_float = cache_blk.astype(jnp.float32)
        scores = jnp.einsum('bhw,bjtw->bhjt', q_float, cache_float) * inv_scale
        positions = page_base + dev_index * PAGE_LEN
        is_valid = positions[None, :, :] < ctx_len[:, None, None]
        scores = jnp.where(is_valid[:, None, :, :], scores, -1e30)
        row_max = jnp.max(scores, axis=(2, 3))
        weights_exp = jnp.exp(scores - row_max[:, :, None, None])
        denom_sum = jnp.sum(weights_exp, axis=(2, 3))
        weights_low = weights_exp.astype(jnp.bfloat16).astype(jnp.float32)
        pv_sum = jnp.einsum('bhjt,bjtc->bhc', weights_low, cache_float[..., :LATENT_DIM])
        part_out = (pv_sum / denom_sum[:, :, None]).astype(jnp.bfloat16)
        part_lse = row_max + jnp.log(denom_sum)
        return part_out, part_lse

    part_outs, part_lses = lax.map(one_device, (jnp.arange(GROUP_SIZE), per_device))
    total_lse = jax.nn.logsumexp(part_lses, axis=0)
    merge_weights = jnp.exp(part_lses - total_lse[None])
    merged = jnp.sum(merge_weights[..., None] * part_outs.astype(jnp.float32), axis=0)
    return merged.astype(jnp.bfloat16)
```

```python
import functools

import jax
import jax.numpy as jnp
from jax import lax
from jax.experimental import pallas as pl
from jax.experimental.pallas import tpu as pltpu
from jax.sharding import PartitionSpec as P

ROPE_DIM = 64
QK_DIM = 192
CORES = 2
SLOTS = 4
AHEAD = 3
F32 = jnp.float32


def columns(row):
    return jnp.transpose(jnp.broadcast_to(row, (row.shape[1], row.shape[1])))


def weights(*lses):
    top = functools.reduce(jnp.maximum, lses)
    exps = [jnp.exp(one - top) for one in lses]
    total = functools.reduce(jnp.add, exps)
    return [columns(one / total) for one in exps], top + jnp.log(total)


def scaled(col, block):
    width = col.shape[1]
    return jnp.concatenate(
        [col * block[:, i : i + width] for i in range(0, block.shape[1], width)], axis=1
    )


def kernel(
    group, len_ref, q_hbm, c_hbm, out_hbm,
    qbuf, cbuf, osend, lsend, orecv, lrecv, own, lown, part, lpart, frecv, flrecv, drecv, dlrecv, outbuf,
    csem, qsem, ag_send, ag_recv, sib_send, sib_recv, ring_send, ring_recv, out_sem,
):
    rounds = qbuf.shape[0]
    chips = group // CORES
    steps = rounds * chips
    seqs = steps * CORES
    latent = osend.shape[2]
    half = latent // 2
    pages, width, page_len = cbuf.shape[1:]
    me = lax.axis_index('dcp')
    chip, core = me // CORES, me % CORES
    sibling = chip * CORES + 1 - core
    right = ((chip + 1) % chips) * CORES + core
    left = ((chip + chips - 1) % chips) * CORES + core
    far = ((chip + 2) % chips) * CORES + core

    def remote(src, dst, send, recv, target):
        return pltpu.make_async_remote_copy(
            src_ref=src, dst_ref=dst, send_sem=send, recv_sem=recv,
            device_id={'dcp': target}, device_id_type=pl.DeviceIdType.MESH)

    def place(n, other):
        r, k = n // chips, n % chips
        dest_chip = (chip + 2 - k + chips) % chips
        dest_core = (1 - core) if other else core
        return r, dest_chip * CORES + dest_core

    def fetch(n, e):
        r, d = place(n, e == 0)
        slot = (2 * n + e) % SLOTS
        return pltpu.make_async_copy(c_hbm.at[d, r, :, 0], cbuf.at[slot], csem.at[slot])

    def q_own(r):
        return pltpu.make_async_copy(q_hbm.at[:, r], qbuf.at[r, me], qsem.at[r])

    def q_copy(r, kind, block, target):
        return remote(qbuf.at[r, block], qbuf.at[r, block], ag_send.at[r, kind], ag_recv.at[r, kind], target)

    def q_first(r):
        q_copy(r, 0, me, right).start()
        q_copy(r, 1, me, left).start()
        q_copy(r, 3, me, sibling).start()

    def q_second(r):
        q_copy(r, 0, left, right).wait_recv()
        q_copy(r, 1, right, left).wait_recv()

        @pl.when(r % 2 == 0)
        def _():
            q_copy(r, 2, left, right).start()

        @pl.when(r % 2 == 1)
        def _():
            q_copy(r, 2, right, left).start()

        q_copy(r, 4, left, sibling).start()
        q_copy(r, 5, right, sibling).start()

    def q_third(r):
        q_copy(r, 2, far, right).wait_recv()
        q_copy(r, 6, far, sibling).start()

    def q_last(r):
        for kind in range(3, 7):
            q_copy(r, kind, me, sibling).wait_recv()

    def attend(n, e):
        r, d = place(n, e == 0)
        slot = (2 * n + e) % SLOTS
        fetch(n, e).wait()
        nxt = 2 * n + e + SLOTS - 1

        @pl.when(nxt < seqs)
        def _():
            fetch((2 * n + e + SLOTS - 1) // 2, (e + SLOTS - 1) % 2).start()

        heads = qbuf.shape[1] * qbuf.shape[3]
        q = qbuf[r, :, d].reshape(heads, width)
        length = len_ref[d * rounds + r]
        scores = []
        for j in range(pages):
            s = jnp.dot(q, cbuf[slot, j], preferred_element_type=F32) * (QK_DIM ** -0.5)
            pos = lax.broadcasted_iota(jnp.int32, s.shape, 1) + (j * group + me) * page_len
            scores.append(jnp.where(pos < length, s, -1e30))
        top = functools.reduce(jnp.maximum, [jnp.max(s, axis=1, keepdims=True) for s in scores])
        exps = [jnp.exp(s - top) for s in scores]
        total = functools.reduce(jnp.add, [jnp.sum(w, axis=1, keepdims=True) for w in exps])
        acc = functools.reduce(jnp.add, [
            lax.dot_general(w.astype(jnp.bfloat16), cbuf[slot, j, :latent], (((1,), (1,)), ((), ())),
                            preferred_element_type=F32)
            for j, w in enumerate(exps)])
        lse = top + jnp.log(total)
        lse = jnp.transpose(jnp.broadcast_to(lse, (heads, heads)))[0:1]
        return (acc / total).astype(jnp.bfloat16), lse

    def sib_o(n):
        return remote(osend.at[n], orecv.at[n], sib_send.at[n, 0], sib_recv.at[n, 0], sibling)

    def sib_l(n):
        return remote(lsend.at[n], lrecv.at[n], sib_send.at[n, 1], sib_recv.at[n, 1], sibling)

    def ring(r, kind):
        target = right if kind % 2 == 0 else left
        k = (0, 0, 1, 3, 1, 3)[kind]
        h = (0, 1, 1, 0, 0, 1)[kind]
        if kind < 2:
            dst, ldst = frecv.at[r, h], flrecv.at[r, h]
        else:
            side = kind % 2
            dst, ldst = drecv.at[r, side, h], dlrecv.at[r, side, h]
        return (
            remote(part.at[r, k, h], dst, ring_send.at[r, kind, 0], ring_recv.at[r, kind, 0], target),
            remote(lpart.at[r, k, h], ldst, ring_send.at[r, kind, 1], ring_recv.at[r, kind, 1], target),
        )

    def ring_start(r, kind):
        for copy in ring(r, kind):
            copy.start()

    def merge(n):
        r, k = n // chips, n % chips
        sib_o(n).wait_recv()
        sib_l(n).wait_recv()
        slot = n % 2
        (wa, wb), lse = weights(lown[slot], lrecv[n])
        for h in range(2):
            cols = pl.ds(h * half, half)
            part[r, k, h] = scaled(wa, own[slot, :, cols].astype(F32)) + scaled(wb, orecv[n, :, cols].astype(F32))
            lpart[r, k, h] = lse

        @pl.when(k == 0)
        def _():
            ring_start(r, 0)
            ring_start(r, 1)

        @pl.when(k == 1)
        def _():
            ring_start(r, 2)

        @pl.when(k == 3)
        def _():
            ring_start(r, 3)

    def relay(r):
        for kind in (4, 5):
            h = kind % 2
            k = (1, 3)[h]
            for copy in ring(r, h):
                copy.wait_recv()
            (wa, wb), lse = weights(lpart[r, k, h], flrecv[r, h])
            part[r, k, h] = scaled(wa, part[r, k, h]) + scaled(wb, frecv[r, h])
            lpart[r, k, h] = lse
            ring_start(r, kind)

    def out_copy(r):
        return pltpu.make_async_copy(outbuf.at[r], out_hbm.at[r], out_sem.at[r])

    def finish(r):
        for kind in (2, 3, 4, 5):
            for copy in ring(r, kind):
                copy.wait_recv()
        for h in range(2):
            (wa, wb, wc), _ = weights(lpart[r, 2, h], dlrecv[r, 0, h], dlrecv[r, 1, h])
            outbuf[r, :, pl.ds(h * half, half)] = (
                scaled(wa, part[r, 2, h]) + scaled(wb, drecv[r, 0, h]) + scaled(wc, drecv[r, 1, h])
            ).astype(jnp.bfloat16)
        out_copy(r).start()

    for r in range(rounds):
        q_own(r).start()
    for u in range(SLOTS - 1):
        fetch(u // 2, u % 2).start()
    barrier = pltpu.get_barrier_semaphore()
    for neighbour in (left, right, sibling):
        pl.semaphore_signal(barrier, inc=1, device_id={'dcp': neighbour}, device_id_type=pl.DeviceIdType.MESH)
    pl.semaphore_wait(barrier, 3)
    for r in range(rounds):
        q_own(r).wait()
    for r in range(AHEAD):
        q_first(r)
    q_second(0)
    q_first(AHEAD)
    q_second(1)
    q_first(AHEAD + 1)
    q_third(0)

    @pl.loop(0, rounds)
    def _(r):
        @pl.when(r + 2 < rounds)
        def _():
            q_second(r + 2)

        @pl.when(r + AHEAD + 2 < rounds)
        def _():
            q_first(r + AHEAD + 2)

        @pl.when(r + 1 < rounds)
        def _():
            q_third(r + 1)

        q_last(r)

        @pl.loop(0, chips)
        def _(k):
            n = r * chips + k
            o, lse = attend(n, 0)
            osend[n] = o
            lsend[n] = lse
            sib_o(n).start()
            sib_l(n).start()
            o, lse = attend(n, 1)
            own[n % 2] = o
            lown[n % 2] = lse

            @pl.when(n >= 1)
            def _():
                merge(n - 1)

        @pl.when(r >= 1)
        def _():
            relay(r - 1)

    merge(steps - 1)
    relay(rounds - 1)

    @pl.loop(0, rounds)
    def _(r):
        finish(r)

    @pl.loop(0, rounds)
    def _(r):
        out_copy(r).wait()
        for kind in range(6):
            for copy in ring(r, kind):
                copy.wait_send()
        q_copy(r, 0, me, right).wait_send()
        q_copy(r, 1, me, left).wait_send()
        for kind in range(2, 7):
            q_copy(r, kind, me, sibling).wait_send()

    @pl.loop(0, steps)
    def _(n):
        sib_o(n).wait_send()
        sib_l(n).wait_send()


def solution(mesh):
    group = mesh.shape['dcp']
    chips = group // CORES

    def local_step(q_blk, cache_blk, len_blk):
        batch, own_heads, width = q_blk.shape
        pages, page_len = cache_blk.shape[1], cache_blk.shape[3]
        latent = width - ROPE_DIM
        half = latent // 2
        rounds = batch // group
        heads = own_heads * group
        steps = rounds * chips
        q = q_blk.reshape(group, rounds, own_heads, width)
        cache = jnp.swapaxes(cache_blk, 3, 4).reshape(group, rounds, pages, 1, width, page_len)
        bf16 = jnp.bfloat16
        dma = pltpu.SemaphoreType.DMA
        return pl.pallas_call(
            functools.partial(kernel, group),
            out_shape=jax.ShapeDtypeStruct((rounds, heads, latent), bf16),
            in_specs=[
                pl.BlockSpec(memory_space=pltpu.SMEM),
                pl.BlockSpec(memory_space=pl.ANY),
                pl.BlockSpec(memory_space=pl.ANY),
            ],
            out_specs=pl.BlockSpec(memory_space=pl.ANY),
            scratch_shapes=[
                pltpu.VMEM((rounds, group, group, own_heads, width), bf16),
                pltpu.VMEM((SLOTS, pages, width, page_len), bf16),
                pltpu.VMEM((steps, heads, latent), bf16),
                pltpu.VMEM((steps, 1, heads), F32),
                pltpu.VMEM((steps, heads, latent), bf16),
                pltpu.VMEM((steps, 1, heads), F32),
                pltpu.VMEM((2, heads, latent), bf16),
                pltpu.VMEM((2, 1, heads), F32),
                pltpu.VMEM((rounds, chips, 2, heads, half), F32),
                pltpu.VMEM((rounds, chips, 2, 1, heads), F32),
                pltpu.VMEM((rounds, 2, heads, half), F32),
                pltpu.VMEM((rounds, 2, 1, heads), F32),
                pltpu.VMEM((rounds, 2, 2, heads, half), F32),
                pltpu.VMEM((rounds, 2, 2, 1, heads), F32),
                pltpu.VMEM((rounds, heads, latent), bf16),
                dma((SLOTS,)),
                dma((rounds,)),
                dma((rounds, 7)),
                dma((rounds, 7)),
                dma((steps, 2)),
                dma((steps, 2)),
                dma((rounds, 6, 2)),
                dma((rounds, 6, 2)),
                dma((rounds,)),
            ],
            compiler_params=pltpu.CompilerParams(
                collective_id=0, has_side_effects=True, vmem_limit_bytes=60000 * 1024),
        )(len_blk, q, cache)

    return jax.shard_map(
        local_step, mesh=mesh,
        in_specs=(P('dp', 'dcp', None), P('dp', None, 'dcp', None, None), P('dp')),
        out_specs=P(('dp', 'dcp'), None, None), check_vma=False)
```

```python
import functools

import jax
import jax.numpy as jnp
from jax import lax
from jax.experimental import pallas as pl
from jax.experimental.pallas import tpu as pltpu
from jax.sharding import PartitionSpec as P

ROPE_DIM = 64
QK_DIM = 192
CORES = 2
SLOTS = 4
AHEAD = 3
LANES = 128
VMEM_BYTES = 46 * 2**20
F32 = jnp.float32


def columns(row):
    return jnp.transpose(jnp.broadcast_to(row, (row.shape[1], row.shape[1])))


def weights(*lses):
    top = functools.reduce(jnp.maximum, lses)
    exps = [jnp.exp(one - top) for one in lses]
    total = functools.reduce(jnp.add, exps)
    return [columns(one / total) for one in exps], top + jnp.log(total)


def scaled(col, block):
    width = col.shape[1]
    return jnp.concatenate(
        [col * block[:, i : i + width] for i in range(0, block.shape[1], width)], axis=1
    )


def kernel(
    group, len_hbm, q_hbm, c_hbm, out_ref,
    len_ref, rope, qbuf, cbuf, osend, lsend, orecv, lrecv, own, lown, part, lpart, frecv, flrecv, drecv, dlrecv,
    lensem, csem, qsem, ag_send, ag_recv, sib_send, sib_recv, ring_send, f_recv, d_recv,
):
    rounds, _, tiles, own_heads, lanes = qbuf.shape
    chips = group // CORES
    steps = rounds * chips
    seqs = steps * CORES
    latent = osend.shape[2]
    half = latent // 2
    pages, width, page_len = cbuf.shape[1:]
    me = lax.axis_index('dcp')
    chip, core = me // CORES, me % CORES
    sibling = chip * CORES + 1 - core
    right = ((chip + 1) % chips) * CORES + core
    left = ((chip + chips - 1) % chips) * CORES + core
    far = ((chip + 2) % chips) * CORES + core

    def remote(src, dst, send, recv, target):
        return pltpu.make_async_remote_copy(
            src_ref=src, dst_ref=dst, send_sem=send, recv_sem=recv,
            device_id={'dcp': target}, device_id_type=pl.DeviceIdType.MESH)

    def place(n, other):
        r, k = n // chips, n % chips
        dest_chip = (chip + 2 - k + chips) % chips
        dest_core = (1 - core) if other else core
        return r, dest_chip * CORES + dest_core

    def fetch(n, e):
        r, d = place(n, e == 0)
        slot = (2 * n + e) % SLOTS
        return pltpu.make_async_copy(c_hbm.at[d, r, :, 0], cbuf.at[slot], csem.at[slot])

    latent_tiles = group * latent // lanes

    def q_load():
        yield pltpu.make_async_copy(q_hbm.at[:, :, :, latent:], rope, qsem.at[1])
        for c in range(latent // lanes):
            for r in range(rounds):
                yield pltpu.make_async_copy(
                    q_hbm.at[:, r, :, c * lanes : (c + 1) * lanes], qbuf.at[r, me, c * group : (c + 1) * group], qsem.at[0])

    def q_pack():
        pltpu.make_async_copy(rope, rope, qsem.at[1]).wait()
        for r in range(rounds):
            for p in range(group // 2):
                qbuf[r, me, latent_tiles + p] = jnp.concatenate([rope[2 * p, r], rope[2 * p + 1, r]], axis=1)
        whole = qbuf.at[:, me, 0:latent_tiles]
        pltpu.make_async_copy(whole, whole, qsem.at[0]).wait()

    def q_copy(r, kind, block, target):
        return remote(qbuf.at[r, block], qbuf.at[r, block], ag_send.at[0], ag_recv.at[r, kind], target)

    def q_wait(r, kind, blocks):
        ref = qbuf.at[r, 0:blocks]
        pltpu.make_async_copy(ref, ref, ag_recv.at[r, kind]).wait()

    def q_first(r):
        q_copy(r, 0, me, right).start()
        q_copy(r, 0, me, left).start()
        q_copy(r, 2, me, sibling).start()

    def q_second(r):
        q_wait(r, 0, 2)

        @pl.when(r % 2 == 0)
        def _():
            q_copy(r, 1, left, right).start()

        @pl.when(r % 2 == 1)
        def _():
            q_copy(r, 1, right, left).start()

        q_copy(r, 2, left, sibling).start()
        q_copy(r, 2, right, sibling).start()

    def q_third(r):
        q_wait(r, 1, 1)
        q_copy(r, 2, far, sibling).start()

    def q_last(r):
        q_wait(r, 2, chips)

    def attend(n, e):
        r, d = place(n, e == 0)
        slot = (2 * n + e) % SLOTS
        fetch(n, e).wait()
        nxt = 2 * n + e + SLOTS - 1

        @pl.when(nxt < seqs)
        def _():
            fetch((2 * n + e + SLOTS - 1) // 2, (e + SLOTS - 1) % 2).start()

        heads = group * own_heads
        q = [qbuf[r, :, c * group + d].reshape(heads, lanes) for c in range(latent // lanes)]
        pair = qbuf[r, :, latent_tiles + d // 2].reshape(heads, lanes)
        q.append(jnp.where(d % 2 == 0, pair[:, : lanes // 2], pair[:, lanes // 2 :]))
        q = jnp.concatenate(q, axis=1)
        length = len_ref[d * rounds + r]
        scores = []
        for j in range(pages):
            s = jnp.dot(q, cbuf[slot, j], preferred_element_type=F32) * (QK_DIM ** -0.5)
            pos = lax.broadcasted_iota(jnp.int32, s.shape, 1) + (j * group + me) * page_len
            scores.append(jnp.where(pos < length, s, -1e30))
        top = functools.reduce(jnp.maximum, [jnp.max(s, axis=1, keepdims=True) for s in scores])
        exps = [jnp.exp(s - top) for s in scores]
        total = functools.reduce(jnp.add, [jnp.sum(w, axis=1, keepdims=True) for w in exps])
        acc = functools.reduce(jnp.add, [
            lax.dot_general(w.astype(jnp.bfloat16), cbuf[slot, j, :latent], (((1,), (1,)), ((), ())),
                            preferred_element_type=F32)
            for j, w in enumerate(exps)])
        lse = top + jnp.log(total)
        lse = jnp.transpose(jnp.broadcast_to(lse, (heads, heads)))[0:1]
        return (acc / total).astype(jnp.bfloat16), lse

    def sib_o(n):
        return remote(osend.at[n], orecv.at[n], sib_send.at[0], sib_recv.at[n % 4, 0], sibling)

    def sib_l(n):
        return remote(lsend.at[n], lrecv.at[n], sib_send.at[1], sib_recv.at[n % 4, 1], sibling)

    def ring(r, kind):
        target = right if kind % 2 == 0 else left
        k = (0, 0, 1, 3, 1, 3)[kind]
        h = (0, 1, 1, 0, 0, 1)[kind]
        if kind < 2:
            dst, ldst, sem = frecv.at[r, h], flrecv.at[r, h], f_recv.at[r % 4, h]
        else:
            side = kind % 2
            dst, ldst, sem = drecv.at[r, side, h], dlrecv.at[r, side, h], d_recv.at[r]
        return (
            remote(part.at[r, k, h], dst, ring_send.at[0], sem.at[0], target),
            remote(lpart.at[r, k, h], ldst, ring_send.at[1], sem.at[1], target),
        )

    def ring_start(r, kind):
        for copy in ring(r, kind):
            copy.start()

    def merge(n):
        r, k = n // chips, n % chips
        sib_o(n).wait_recv()
        sib_l(n).wait_recv()
        slot = n % 2
        (wa, wb), lse = weights(lown[slot], lrecv[n])
        for h in range(2):
            cols = pl.ds(h * half, half)
            part[r, k, h] = scaled(wa, own[slot, :, cols].astype(F32)) + scaled(wb, orecv[n, :, cols].astype(F32))
            lpart[r, k, h] = lse

        @pl.when(k == 0)
        def _():
            ring_start(r, 0)
            ring_start(r, 1)

        @pl.when(k == 1)
        def _():
            ring_start(r, 2)

        @pl.when(k == 3)
        def _():
            ring_start(r, 3)

    def relay(r):
        for kind in (4, 5):
            h = kind % 2
            k = (1, 3)[h]
            for copy in ring(r, h):
                copy.wait_recv()
            (wa, wb), lse = weights(lpart[r, k, h], flrecv[r, h])
            part[r, k, h] = scaled(wa, part[r, k, h]) + scaled(wb, frecv[r, h])
            lpart[r, k, h] = lse
            ring_start(r, kind)

    def finish(r):
        pltpu.make_async_copy(drecv.at[r], drecv.at[r], d_recv.at[r, 0]).wait()
        pltpu.make_async_copy(dlrecv.at[r], dlrecv.at[r], d_recv.at[r, 1]).wait()
        for h in range(2):
            (wa, wb, wc), _ = weights(lpart[r, 2, h], dlrecv[r, 0, h], dlrecv[r, 1, h])
            out_ref[r, :, pl.ds(h * half, half)] = (
                scaled(wa, part[r, 2, h]) + scaled(wb, drecv[r, 0, h]) + scaled(wc, drecv[r, 1, h])
            ).astype(jnp.bfloat16)

    for copy in q_load():
        copy.start()
    len_copy = pltpu.make_async_copy(len_hbm, len_ref, lensem)
    len_copy.start()
    for u in range(SLOTS - 1):
        fetch(u // 2, u % 2).start()
    barrier = pltpu.get_barrier_semaphore()
    for neighbour in (left, right, sibling):
        pl.semaphore_signal(barrier, inc=1, device_id={'dcp': neighbour}, device_id_type=pl.DeviceIdType.MESH)
    q_pack()
    len_copy.wait()
    pl.semaphore_wait(barrier, 3)
    for r in range(AHEAD):
        q_first(r)
    q_second(0)
    q_first(AHEAD)
    q_second(1)
    q_first(AHEAD + 1)
    q_third(0)

    @pl.loop(0, rounds)
    def _(r):
        @pl.when(r + 2 < rounds)
        def _():
            q_second(r + 2)

        @pl.when(r + AHEAD + 2 < rounds)
        def _():
            q_first(r + AHEAD + 2)

        @pl.when(r + 1 < rounds)
        def _():
            q_third(r + 1)

        q_last(r)

        @pl.loop(0, chips)
        def _(k):
            n = r * chips + k
            o, lse = attend(n, 0)
            osend[n] = o
            lsend[n] = lse
            sib_o(n).start()
            sib_l(n).start()
            o, lse = attend(n, 1)
            own[n % 2] = o
            lown[n % 2] = lse

            @pl.when(n >= 1)
            def _():
                merge(n - 1)

        @pl.when(r >= 1)
        def _():
            relay(r - 1)

    merge(steps - 1)
    relay(rounds - 1)

    @pl.loop(0, rounds)
    def _(r):
        finish(r)

    def sent(ref, sem):
        pltpu.make_async_copy(ref, ref, sem).wait()

    sent(qbuf.at[:, 0:7], ag_send.at[0])
    sent(osend, sib_send.at[0])
    sent(lsend, sib_send.at[1])
    sent(part.at[:, 0:3], ring_send.at[0])
    sent(lpart.at[:, 0:3], ring_send.at[1])


def put_out(src_ref, dst_ref, sem):
    copy = pltpu.make_async_copy(src_ref, dst_ref, sem)
    copy.start()
    copy.wait()


def solution(mesh):
    group = mesh.shape['dcp']
    chips = group // CORES

    def local_step(q_blk, cache_blk, len_blk):
        batch, own_heads, width = q_blk.shape
        pages, page_len = cache_blk.shape[1], cache_blk.shape[3]
        latent = width - ROPE_DIM
        half = latent // 2
        rounds = batch // group
        heads = own_heads * group
        steps = rounds * chips
        q = q_blk.reshape(group, rounds, own_heads, width)
        cache = jnp.swapaxes(cache_blk, 3, 4).reshape(group, rounds, pages, 1, width, page_len)
        bf16 = jnp.bfloat16
        dma = pltpu.SemaphoreType.DMA
        tiles = group * latent // LANES + group // 2
        hbm = pl.BlockSpec(memory_space=pltpu.HBM)
        vmem = pl.BlockSpec(memory_space=pltpu.VMEM)
        out = jax.ShapeDtypeStruct((rounds, heads, latent), bf16)
        merged = pl.pallas_call(
            functools.partial(kernel, group),
            out_shape=out,
            in_specs=[hbm, hbm, hbm],
            out_specs=vmem,
            scratch_shapes=[
                pltpu.SMEM((batch,), jnp.int32),
                pltpu.VMEM((group, rounds, own_heads, ROPE_DIM), bf16),
                pltpu.VMEM((rounds, group, tiles, own_heads, LANES), bf16),
                pltpu.VMEM((SLOTS, pages, width, page_len), bf16),
                pltpu.VMEM((steps, heads, latent), bf16),
                pltpu.VMEM((steps, 1, heads), F32),
                pltpu.VMEM((steps, heads, latent), bf16),
                pltpu.VMEM((steps, 1, heads), F32),
                pltpu.VMEM((2, heads, latent), bf16),
                pltpu.VMEM((2, 1, heads), F32),
                pltpu.VMEM((rounds, chips, 2, heads, half), F32),
                pltpu.VMEM((rounds, chips, 2, 1, heads), F32),
                pltpu.VMEM((rounds, 2, heads, half), F32),
                pltpu.VMEM((rounds, 2, 1, heads), F32),
                pltpu.VMEM((rounds, 2, 2, heads, half), F32),
                pltpu.VMEM((rounds, 2, 2, 1, heads), F32),
                dma,
                dma((SLOTS,)),
                dma((2,)),
                dma((1,)),
                dma((rounds, 3)),
                dma((2,)),
                dma((4, 2)),
                dma((2,)),
                dma((4, 2, 2)),
                dma((rounds, 2)),
            ],
            compiler_params=pltpu.CompilerParams(
                collective_id=0, has_side_effects=True, vmem_limit_bytes=VMEM_BYTES),
        )(*(pltpu.with_memory_space_constraint(x, pltpu.HBM) for x in (len_blk, q, cache)))
        return pl.pallas_call(
            put_out, out_shape=out, in_specs=[vmem], out_specs=hbm, scratch_shapes=[dma],
            compiler_params=pltpu.CompilerParams(vmem_limit_bytes=VMEM_BYTES),
        )(merged)

    return jax.shard_map(
        local_step, mesh=mesh,
        in_specs=(P('dp', 'dcp', None), P('dp', None, 'dcp', None, None), P('dp')),
        out_specs=P(('dp', 'dcp'), None, None), check_vma=False)
```

```python
import functools

import jax
import jax.numpy as jnp
from jax import lax
from jax.experimental import pallas as pl
from jax.experimental.pallas import tpu as pltpu
from jax.sharding import PartitionSpec as P

ROPE_DIM = 64
QK_DIM = 192
CORES = 2
SLOTS = 4
AHEAD = 3
LANES = 128
VMEM_BYTES = 46 * 2**20
F32 = jnp.float32


def columns(row):
    return jnp.transpose(jnp.broadcast_to(row, (row.shape[1], row.shape[1])))


def weights(*lses):
    top = functools.reduce(jnp.maximum, lses)
    exps = [jnp.exp(one - top) for one in lses]
    total = functools.reduce(jnp.add, exps)
    return [columns(one / total) for one in exps], top + jnp.log(total)


def kernel(
    group, len_hbm, q_hbm, c_hbm, out_ref,
    len_ref, rope, qbuf, cbuf, osend, lsend, orecv, lrecv, own, lown, part, frecv, drecv,
    lensem, csem, qsem, ag_send, ag_recv, sib_send, sib_recv, ring_send, f_recv, d_recv,
):
    rounds, _, tiles, own_heads, lanes = qbuf.shape
    chips = group // CORES
    steps = rounds * chips
    seqs = steps * CORES
    heads, latent = osend.shape[1:]
    blocks = latent // lanes // 2
    lse_row = pl.ds(blocks * heads, 1)
    rows = pl.ds(0, blocks * heads + 1)

    def block_rows(i):
        return pl.ds(i * heads, heads)
    pages, width, page_len = cbuf.shape[1:]
    me = lax.axis_index('dcp')
    chip, core = me // CORES, me % CORES
    sibling = chip * CORES + 1 - core
    right = ((chip + 1) % chips) * CORES + core
    left = ((chip + chips - 1) % chips) * CORES + core
    far = ((chip + 2) % chips) * CORES + core

    def remote(src, dst, send, recv, target):
        return pltpu.make_async_remote_copy(
            src_ref=src, dst_ref=dst, send_sem=send, recv_sem=recv,
            device_id={'dcp': target}, device_id_type=pl.DeviceIdType.MESH)

    def wait_bytes(ref, sem):
        pltpu.make_async_copy(ref, ref, sem).wait()

    def place(n, other):
        r, k = n // chips, n % chips
        dest_chip = (chip + 2 - k + chips) % chips
        dest_core = (1 - core) if other else core
        return r, dest_chip * CORES + dest_core

    def fetch(n, e):
        r, d = place(n, e == 0)
        slot = (2 * n + e) % SLOTS
        return pltpu.make_async_copy(c_hbm.at[d, r, :, 0], cbuf.at[slot], csem.at[slot])

    latent_tiles = group * latent // lanes

    def q_load():
        yield pltpu.make_async_copy(q_hbm.at[:, :, :, latent:], rope, qsem.at[2])
        for r in range(rounds):
            for c in range(latent // lanes):
                yield pltpu.make_async_copy(
                    q_hbm.at[:, r, :, c * lanes : (c + 1) * lanes], qbuf.at[r, me, c * group : (c + 1) * group],
                    qsem.at[min(r, 1)])

    def q_pack(r):
        for p in range(group // 2):
            qbuf[r, me, latent_tiles + p] = jnp.concatenate([rope[2 * p, r], rope[2 * p + 1, r]], axis=1)

    def q_copy(r, kind, block, target):
        return remote(qbuf.at[r, block], qbuf.at[r, block], ag_send, ag_recv.at[r, kind], target)

    def q_wait(r, kind, count):
        wait_bytes(qbuf.at[r, 0:count], ag_recv.at[r, kind])

    def q_first(r):
        q_copy(r, 0, me, right).start()
        q_copy(r, 0, me, left).start()
        q_copy(r, 2, me, sibling).start()

    def q_second(r):
        q_wait(r, 0, 2)

        @pl.when(r % 2 == 0)
        def _():
            q_copy(r, 1, left, right).start()

        @pl.when(r % 2 == 1)
        def _():
            q_copy(r, 1, right, left).start()

        q_copy(r, 2, left, sibling).start()
        q_copy(r, 2, right, sibling).start()

    def q_third(r):
        q_wait(r, 1, 1)
        q_copy(r, 2, far, sibling).start()

    def q_last(r):
        q_wait(r, 2, chips)

    def attend(n, e):
        r, d = place(n, e == 0)
        slot = (2 * n + e) % SLOTS
        fetch(n, e).wait()
        nxt = 2 * n + e + SLOTS - 1

        @pl.when(nxt < seqs)
        def _():
            fetch((2 * n + e + SLOTS - 1) // 2, (e + SLOTS - 1) % 2).start()

        q = [qbuf[r, :, c * group + d].reshape(heads, lanes) for c in range(latent // lanes)]
        pair = qbuf[r, :, latent_tiles + d // 2].reshape(heads, lanes)
        q.append(jnp.where(d % 2 == 0, pair[:, : lanes // 2], pair[:, lanes // 2 :]))
        q = jnp.concatenate(q, axis=1)
        length = len_ref[d * rounds + r]
        scores = []
        for j in range(pages):
            s = jnp.dot(q, cbuf[slot, j], preferred_element_type=F32) * (QK_DIM ** -0.5)
            pos = lax.broadcasted_iota(jnp.int32, s.shape, 1) + (j * group + me) * page_len
            scores.append(jnp.where(pos < length, s, -1e30))
        top = functools.reduce(jnp.maximum, [jnp.max(s, axis=1, keepdims=True) for s in scores])
        exps = [jnp.exp(s - top) for s in scores]
        total = functools.reduce(jnp.add, [jnp.sum(w, axis=1, keepdims=True) for w in exps])
        acc = functools.reduce(jnp.add, [
            lax.dot_general(w.astype(jnp.bfloat16), cbuf[slot, j, :latent], (((1,), (1,)), ((), ())),
                            preferred_element_type=F32)
            for j, w in enumerate(exps)])
        lse = top + jnp.log(total)
        lse = jnp.transpose(jnp.broadcast_to(lse, (heads, heads)))[0:1]
        return (acc / total).astype(jnp.bfloat16), lse

    def sib_o(n):
        return remote(osend.at[n], orecv.at[n], sib_send.at[0], sib_recv.at[n % 4, 0], sibling)

    def sib_l(n):
        return remote(lsend.at[n], lrecv.at[n], sib_send.at[1], sib_recv.at[n % 4, 1], sibling)

    def ring(r, kind):
        target = right if kind % 2 == 0 else left
        k = (0, 0, 1, 3, 1, 3)[kind]
        h = (0, 1, 1, 0, 0, 1)[kind]
        if kind < 2:
            dst, sem = frecv.at[r, h, rows], f_recv.at[r % 4, h]
        else:
            dst, sem = drecv.at[r, kind % 2, h, rows], d_recv.at[r]
        return remote(part.at[r, k, h, rows], dst, ring_send, sem, target)

    def merge(n):
        r, k = n // chips, n % chips
        sib_o(n).wait_recv()
        sib_l(n).wait_recv()
        slot = n % 2
        (wa, wb), lse = weights(lown[slot], lrecv[n])
        for h in range(2):
            for i in range(blocks):
                cols = pl.ds((h * blocks + i) * lanes, lanes)
                part[r, k, h, block_rows(i)] = wa * own[slot, :, cols].astype(F32) + wb * orecv[n, :, cols].astype(F32)
            part[r, k, h, lse_row] = lse

        @pl.when(k == 0)
        def _():
            ring(r, 0).start()
            ring(r, 1).start()

        @pl.when(k == 1)
        def _():
            ring(r, 2).start()

        @pl.when(k == 3)
        def _():
            ring(r, 3).start()

    def relay(r):
        for kind in (4, 5):
            h = kind % 2
            k = (1, 3)[h]
            ring(r, h).wait_recv()
            (wa, wb), lse = weights(part[r, k, h, lse_row], frecv[r, h, lse_row])
            for i in range(blocks):
                part[r, k, h, block_rows(i)] = wa * part[r, k, h, block_rows(i)] + wb * frecv[r, h, block_rows(i)]
            part[r, k, h, lse_row] = lse
            ring(r, kind).start()

    def finish(r):
        wait_bytes(drecv.at[r, :, :, rows], d_recv.at[r])
        for h in range(2):
            parts = [part.at[r, 2, h], drecv.at[r, 0, h], drecv.at[r, 1, h]]
            cols, _ = weights(*(one[lse_row] for one in parts))
            for i in range(blocks):
                total = functools.reduce(jnp.add, [col * one[block_rows(i)] for col, one in zip(cols, parts)])
                out_ref[r, :, pl.ds((h * blocks + i) * lanes, lanes)] = total.astype(jnp.bfloat16)

    for copy in q_load():
        copy.start()
    len_copy = pltpu.make_async_copy(len_hbm, len_ref, lensem)
    len_copy.start()
    for u in range(SLOTS - 1):
        fetch(u // 2, u % 2).start()
    barrier = pltpu.get_barrier_semaphore()
    for neighbour in (left, right, sibling):
        pl.semaphore_signal(barrier, inc=1, device_id={'dcp': neighbour}, device_id_type=pl.DeviceIdType.MESH)
    wait_bytes(rope, qsem.at[2])
    q_pack(0)
    wait_bytes(qbuf.at[0, me, 0:latent_tiles], qsem.at[0])
    pl.semaphore_wait(barrier, 3)
    q_first(0)
    for r in range(1, rounds):
        q_pack(r)
    wait_bytes(qbuf.at[1:rounds, me, 0:latent_tiles], qsem.at[1])
    for r in range(1, AHEAD):
        q_first(r)
    len_copy.wait()
    q_second(0)
    q_first(AHEAD)
    q_second(1)
    q_first(AHEAD + 1)
    q_third(0)

    @pl.loop(0, rounds)
    def _(r):
        @pl.when(r + 2 < rounds)
        def _():
            q_second(r + 2)

        @pl.when(r + AHEAD + 2 < rounds)
        def _():
            q_first(r + AHEAD + 2)

        @pl.when(r + 1 < rounds)
        def _():
            q_third(r + 1)

        q_last(r)

        @pl.loop(0, chips)
        def _(k):
            n = r * chips + k
            o, lse = attend(n, 0)
            osend[n] = o
            lsend[n] = lse
            sib_o(n).start()
            sib_l(n).start()
            o, lse = attend(n, 1)
            own[n % 2] = o
            lown[n % 2] = lse

            @pl.when(n >= 1)
            def _():
                merge(n - 1)

        @pl.when(r >= 1)
        def _():
            relay(r - 1)

    merge(steps - 1)
    relay(rounds - 1)

    @pl.loop(0, rounds)
    def _(r):
        finish(r)

    wait_bytes(qbuf.at[:, 0:7], ag_send)
    wait_bytes(osend, sib_send.at[0])
    wait_bytes(lsend, sib_send.at[1])
    wait_bytes(part.at[:, 0:3, :, rows], ring_send)


def put_out(src_ref, dst_ref, sem):
    copy = pltpu.make_async_copy(src_ref, dst_ref, sem)
    copy.start()
    copy.wait()


def solution(mesh):
    group = mesh.shape['dcp']
    chips = group // CORES

    def local_step(q_blk, cache_blk, len_blk):
        batch, own_heads, width = q_blk.shape
        pages, page_len = cache_blk.shape[1], cache_blk.shape[3]
        latent = width - ROPE_DIM
        rounds = batch // group
        heads = own_heads * group
        steps = rounds * chips
        rows = latent // LANES // 2 * heads + 8
        q = q_blk.reshape(group, rounds, own_heads, width)
        cache = jnp.swapaxes(cache_blk, 3, 4).reshape(group, rounds, pages, 1, width, page_len)
        bf16 = jnp.bfloat16
        dma = pltpu.SemaphoreType.DMA
        tiles = group * latent // LANES + group // 2
        hbm = pl.BlockSpec(memory_space=pltpu.HBM)
        vmem = pl.BlockSpec(memory_space=pltpu.VMEM)
        out = jax.ShapeDtypeStruct((rounds, heads, latent), bf16)
        merged = pl.pallas_call(
            functools.partial(kernel, group),
            out_shape=out,
            in_specs=[hbm, hbm, hbm],
            out_specs=vmem,
            scratch_shapes=[
                pltpu.SMEM((batch,), jnp.int32),
                pltpu.VMEM((group, rounds, own_heads, ROPE_DIM), bf16),
                pltpu.VMEM((rounds, group, tiles, own_heads, LANES), bf16),
                pltpu.VMEM((SLOTS, pages, width, page_len), bf16),
                pltpu.VMEM((steps, heads, latent), bf16),
                pltpu.VMEM((steps, 1, heads), F32),
                pltpu.VMEM((steps, heads, latent), bf16),
                pltpu.VMEM((steps, 1, heads), F32),
                pltpu.VMEM((2, heads, latent), bf16),
                pltpu.VMEM((2, 1, heads), F32),
                pltpu.VMEM((rounds, chips, 2, rows, LANES), F32),
                pltpu.VMEM((rounds, 2, rows, LANES), F32),
                pltpu.VMEM((rounds, 2, 2, rows, LANES), F32),
                dma,
                dma((SLOTS,)),
                dma((3,)),
                dma,
                dma((rounds, 3)),
                dma((2,)),
                dma((4, 2)),
                dma,
                dma((4, 2)),
                dma((rounds,)),
            ],
            compiler_params=pltpu.CompilerParams(
                collective_id=0, has_side_effects=True, vmem_limit_bytes=VMEM_BYTES),
        )(*(pltpu.with_memory_space_constraint(x, pltpu.HBM) for x in (len_blk, q, cache)))
        return pl.pallas_call(
            put_out, out_shape=out, in_specs=[vmem], out_specs=hbm, scratch_shapes=[dma],
            compiler_params=pltpu.CompilerParams(vmem_limit_bytes=VMEM_BYTES),
        )(merged)

    return jax.shard_map(
        local_step, mesh=mesh,
        in_specs=(P('dp', 'dcp', None), P('dp', None, 'dcp', None, None), P('dp')),
        out_specs=P(('dp', 'dcp'), None, None), check_vma=False)
```

```python
import functools

import jax
import jax.numpy as jnp
from jax import lax
from jax.experimental import pallas as pl
from jax.experimental.pallas import tpu as pltpu
from jax.sharding import PartitionSpec as P

ROPE_DIM = 64
QK_DIM = 192
CORES = 2
SLOTS = 4
AHEAD = 3
LANES = 128
VMEM_BYTES = 36 * 2**20
F32 = jnp.float32


def columns(row):
    return jnp.transpose(jnp.broadcast_to(row, (row.shape[1], row.shape[1])))


def weights(*lses):
    top = functools.reduce(jnp.maximum, lses)
    exps = [jnp.exp(one - top) for one in lses]
    total = functools.reduce(jnp.add, exps)
    return [columns(one / total) for one in exps], top + jnp.log(total)


def finish(local, received, out_ref):
    heads, latent = out_ref.shape
    blocks = latent // LANES // 2
    lse_row = pl.ds(blocks * heads, 1)
    for h in range(2):
        parts = [local.at[h], received.at[0, h], received.at[1, h]]
        cols, _ = weights(*(one[lse_row] for one in parts))
        for i in range(blocks):
            rows = pl.ds(i * heads, heads)
            total = functools.reduce(jnp.add, [col * one[rows] for col, one in zip(cols, parts)])
            out_ref[:, pl.ds((h * blocks + i) * LANES, LANES)] = total.astype(jnp.bfloat16)


def kernel(
    group, len_hbm, q_hbm, c_hbm, out_ref, part, drecv,
    len_ref, rope, qbuf, cbuf, osend, lsend, orecv, lrecv, own, lown, frecv,
    lensem, csem, qsem, ag_send, ag_recv, sib_send, sib_recv, ring_send, f_recv, d_recv,
):
    rounds, _, tiles, own_heads, lanes = qbuf.shape
    chips = group // CORES
    steps = rounds * chips
    seqs = steps * CORES
    heads, latent = osend.shape[1:]
    blocks = latent // lanes // 2
    lse_row = pl.ds(blocks * heads, 1)
    rows = pl.ds(0, blocks * heads + 1)

    def block_rows(i):
        return pl.ds(i * heads, heads)
    pages, width, page_len = cbuf.shape[1:]
    me = lax.axis_index('dcp')
    chip, core = me // CORES, me % CORES
    sibling = chip * CORES + 1 - core
    right = ((chip + 1) % chips) * CORES + core
    left = ((chip + chips - 1) % chips) * CORES + core
    far = ((chip + 2) % chips) * CORES + core

    def remote(src, dst, send, recv, target):
        return pltpu.make_async_remote_copy(
            src_ref=src, dst_ref=dst, send_sem=send, recv_sem=recv,
            device_id={'dcp': target}, device_id_type=pl.DeviceIdType.MESH)

    def wait_bytes(ref, sem):
        pltpu.make_async_copy(ref, ref, sem).wait()

    def place(n, other):
        r, k = n // chips, n % chips
        dest_chip = (chip + 2 - k + chips) % chips
        dest_core = (1 - core) if other else core
        return r, dest_chip * CORES + dest_core

    def fetch(n, e):
        r, d = place(n, e == 0)
        slot = (2 * n + e) % SLOTS
        return pltpu.make_async_copy(c_hbm.at[d, r, :, 0], cbuf.at[slot], csem.at[slot])

    latent_tiles = group * latent // lanes

    def q_load():
        yield pltpu.make_async_copy(q_hbm.at[:, 0, :, latent:], rope.at[:, 0], qsem.at[2])
        for r in range(rounds):
            for c in range(latent // lanes):
                yield pltpu.make_async_copy(
                    q_hbm.at[:, r, :, c * lanes : (c + 1) * lanes], qbuf.at[r, me, c * group : (c + 1) * group],
                    qsem.at[min(r, 1)])
            if r == 0:
                yield pltpu.make_async_copy(q_hbm.at[:, 1:, :, latent:], rope.at[:, 1:], qsem.at[3])

    def q_pack(r):
        for p in range(group // 2):
            qbuf[r, me, latent_tiles + p] = jnp.concatenate([rope[2 * p, r], rope[2 * p + 1, r]], axis=1)

    def q_copy(r, kind, block, target):
        return remote(qbuf.at[r, block], qbuf.at[r, block], ag_send, ag_recv.at[r, kind], target)

    def q_wait(r, kind, count):
        wait_bytes(qbuf.at[r, 0:count], ag_recv.at[r, kind])

    def q_first(r):
        q_copy(r, 0, me, right).start()
        q_copy(r, 0, me, left).start()
        q_copy(r, 2, me, sibling).start()

    def q_second(r):
        q_wait(r, 0, 2)

        @pl.when(r % 2 == 0)
        def _():
            q_copy(r, 1, left, right).start()

        @pl.when(r % 2 == 1)
        def _():
            q_copy(r, 1, right, left).start()

        q_copy(r, 2, left, sibling).start()
        q_copy(r, 2, right, sibling).start()

    def q_third(r):
        q_wait(r, 1, 1)
        q_copy(r, 2, far, sibling).start()

    def q_last(r):
        q_wait(r, 2, chips)

    def attend(n, e):
        r, d = place(n, e == 0)
        slot = (2 * n + e) % SLOTS
        fetch(n, e).wait()
        nxt = 2 * n + e + SLOTS - 1

        @pl.when(nxt < seqs)
        def _():
            fetch((2 * n + e + SLOTS - 1) // 2, (e + SLOTS - 1) % 2).start()

        q = [qbuf[r, :, c * group + d].reshape(heads, lanes) for c in range(latent // lanes)]
        pair = qbuf[r, :, latent_tiles + d // 2].reshape(heads, lanes)
        q.append(jnp.where(d % 2 == 0, pair[:, : lanes // 2], pair[:, lanes // 2 :]))
        q = jnp.concatenate(q, axis=1)
        length = len_ref[d * rounds + r]
        scores = []
        for j in range(pages):
            s = jnp.dot(q, cbuf[slot, j], preferred_element_type=F32) * (QK_DIM ** -0.5)
            pos = lax.broadcasted_iota(jnp.int32, s.shape, 1) + (j * group + me) * page_len
            scores.append(jnp.where(pos < length, s, -1e30))
        top = functools.reduce(jnp.maximum, [jnp.max(s, axis=1, keepdims=True) for s in scores])
        exps = [jnp.exp(s - top) for s in scores]
        total = functools.reduce(jnp.add, [jnp.sum(w, axis=1, keepdims=True) for w in exps])
        acc = functools.reduce(jnp.add, [
            lax.dot_general(w.astype(jnp.bfloat16), cbuf[slot, j, :latent], (((1,), (1,)), ((), ())),
                            preferred_element_type=F32)
            for j, w in enumerate(exps)])
        lse = top + jnp.log(total)
        lse = jnp.transpose(jnp.broadcast_to(lse, (heads, heads)))[0:1]
        return (acc / total).astype(jnp.bfloat16), lse

    def sib_o(n):
        return remote(osend.at[n], orecv.at[n], sib_send.at[0], sib_recv.at[n % 4, 0], sibling)

    def sib_l(n):
        return remote(lsend.at[n], lrecv.at[n], sib_send.at[1], sib_recv.at[n % 4, 1], sibling)

    def ring(r, kind):
        target = right if kind % 2 == 0 else left
        k = (0, 0, 1, 3, 1, 3)[kind]
        h = (0, 1, 1, 0, 0, 1)[kind]
        if kind < 2:
            dst, sem = frecv.at[r, h, rows], f_recv.at[r % 4, h]
        else:
            dst, sem = drecv.at[r, kind % 2, h, rows], d_recv.at[r]
        return remote(part.at[r, k, h, rows], dst, ring_send, sem, target)

    def merge(n):
        r, k = n // chips, n % chips
        sib_o(n).wait_recv()
        sib_l(n).wait_recv()
        slot = n % 2
        (wa, wb), lse = weights(lown[slot], lrecv[n])
        for h in range(2):
            for i in range(blocks):
                cols = pl.ds((h * blocks + i) * lanes, lanes)
                part[r, k, h, block_rows(i)] = wa * own[slot, :, cols].astype(F32) + wb * orecv[n, :, cols].astype(F32)
            part[r, k, h, lse_row] = lse

        @pl.when(k == 0)
        def _():
            ring(r, 0).start()
            ring(r, 1).start()

        @pl.when(k == 1)
        def _():
            ring(r, 2).start()

        @pl.when(k == 3)
        def _():
            ring(r, 3).start()

    def relay(r):
        for kind in (4, 5):
            h = kind % 2
            k = (1, 3)[h]
            ring(r, h).wait_recv()
            (wa, wb), lse = weights(part[r, k, h, lse_row], frecv[r, h, lse_row])
            for i in range(blocks):
                part[r, k, h, block_rows(i)] = wa * part[r, k, h, block_rows(i)] + wb * frecv[r, h, block_rows(i)]
            part[r, k, h, lse_row] = lse
            ring(r, kind).start()

    def arrive(r):
        wait_bytes(drecv.at[r, :, :, rows], d_recv.at[r])

    barrier = pltpu.get_barrier_semaphore()
    for neighbour in (left, right, sibling):
        pl.semaphore_signal(barrier, inc=1, device_id={'dcp': neighbour}, device_id_type=pl.DeviceIdType.MESH)
    for copy in q_load():
        copy.start()
    len_copy = pltpu.make_async_copy(len_hbm, len_ref, lensem)
    len_copy.start()
    for u in range(SLOTS - 1):
        fetch(u // 2, u % 2).start()
    pl.semaphore_wait(barrier, 3)
    for c in range(latent // lanes):
        to = pl.ds(c * group, group)
        for target in (right, left):
            remote(q_hbm.at[:, 0, :, c * lanes : (c + 1) * lanes], qbuf.at[0, me, to], ag_send, ag_recv.at[0, 0], target).start()
    wait_bytes(rope.at[:, 0], qsem.at[2])
    q_pack(0)
    to = pl.ds(latent_tiles, group // 2)
    for target in (right, left):
        remote(qbuf.at[0, me, to], qbuf.at[0, me, to], ag_send, ag_recv.at[0, 0], target).start()
    wait_bytes(qbuf.at[0, me, 0:latent_tiles], qsem.at[0])
    q_copy(0, 2, me, sibling).start()
    wait_bytes(rope.at[:, 1:], qsem.at[3])
    for r in range(1, rounds):
        q_pack(r)
    wait_bytes(qbuf.at[1:rounds, me, 0:latent_tiles], qsem.at[1])
    for r in range(1, AHEAD):
        q_first(r)
    len_copy.wait()
    q_second(0)
    q_first(AHEAD)
    q_second(1)
    q_first(AHEAD + 1)
    q_third(0)

    @pl.loop(0, rounds)
    def _(r):
        @pl.when(r + 2 < rounds)
        def _():
            q_second(r + 2)

        @pl.when(r + AHEAD + 2 < rounds)
        def _():
            q_first(r + AHEAD + 2)

        @pl.when(r + 1 < rounds)
        def _():
            q_third(r + 1)

        q_last(r)

        @pl.loop(0, chips)
        def _(k):
            n = r * chips + k
            o, lse = attend(n, 0)
            osend[n] = o
            lsend[n] = lse
            sib_o(n).start()
            sib_l(n).start()
            o, lse = attend(n, 1)
            own[n % 2] = o
            lown[n % 2] = lse

            @pl.when(n >= 1)
            def _():
                merge(n - 1)

        @pl.when(r >= 1)
        def _():
            relay(r - 1)

    merge(steps - 1)
    relay(rounds - 1)

    @pl.loop(0, rounds - 1)
    def _(r):
        arrive(r)
        finish(part.at[r, 2], drecv.at[r], out_ref.at[r])

    arrive(rounds - 1)

    wait_bytes(qbuf.at[:, 0:7], ag_send)
    wait_bytes(osend, sib_send.at[0])
    wait_bytes(lsend, sib_send.at[1])
    wait_bytes(part.at[:, 0:3, :, rows], ring_send)


def put_out(done, part, drecv, out_hbm, last, sems):
    n = done.shape[0]
    copies = [
        pltpu.make_async_copy(done, out_hbm.at[pl.ds(0, n)], sems.at[0]),
        pltpu.make_async_copy(last, out_hbm.at[n], sems.at[1]),
    ]
    copies[0].start()
    finish(part.at[n, 2], drecv.at[n], last)
    copies[1].start()
    for copy in copies:
        copy.wait()


def solution(mesh):
    group = mesh.shape['dcp']
    chips = group // CORES

    def local_step(q_blk, cache_blk, len_blk):
        batch, own_heads, width = q_blk.shape
        pages, page_len = cache_blk.shape[1], cache_blk.shape[3]
        latent = width - ROPE_DIM
        rounds = batch // group
        heads = own_heads * group
        steps = rounds * chips
        rows = latent // LANES // 2 * heads + 8
        q = q_blk.reshape(group, rounds, own_heads, width)
        cache = jnp.swapaxes(cache_blk, 3, 4).reshape(group, rounds, pages, 1, width, page_len)
        bf16 = jnp.bfloat16
        dma = pltpu.SemaphoreType.DMA
        tiles = group * latent // LANES + group // 2
        hbm = pl.BlockSpec(memory_space=pltpu.HBM)
        vmem = pl.BlockSpec(memory_space=pltpu.VMEM)
        done, part, drecv = pl.pallas_call(
            functools.partial(kernel, group),
            out_shape=[
                jax.ShapeDtypeStruct((rounds - 1, heads, latent), bf16),
                jax.ShapeDtypeStruct((rounds, chips, 2, rows, LANES), F32),
                jax.ShapeDtypeStruct((rounds, 2, 2, rows, LANES), F32),
            ],
            in_specs=[hbm, hbm, hbm],
            out_specs=[vmem] * 3,
            scratch_shapes=[
                pltpu.SMEM((batch,), jnp.int32),
                pltpu.VMEM((group, rounds, own_heads, ROPE_DIM), bf16),
                pltpu.VMEM((rounds, group, tiles, own_heads, LANES), bf16),
                pltpu.VMEM((SLOTS, pages, width, page_len), bf16),
                pltpu.VMEM((steps, heads, latent), bf16),
                pltpu.VMEM((steps, 1, heads), F32),
                pltpu.VMEM((steps, heads, latent), bf16),
                pltpu.VMEM((steps, 1, heads), F32),
                pltpu.VMEM((2, heads, latent), bf16),
                pltpu.VMEM((2, 1, heads), F32),
                pltpu.VMEM((rounds, 2, rows, LANES), F32),
                dma,
                dma((SLOTS,)),
                dma((4,)),
                dma,
                dma((rounds, 3)),
                dma((2,)),
                dma((4, 2)),
                dma,
                dma((4, 2)),
                dma((rounds,)),
            ],
            compiler_params=pltpu.CompilerParams(
                collective_id=0, has_side_effects=True, vmem_limit_bytes=VMEM_BYTES),
        )(*(pltpu.with_memory_space_constraint(x, pltpu.HBM) for x in (len_blk, q, cache)))
        return pl.pallas_call(
            put_out,
            out_shape=jax.ShapeDtypeStruct((rounds, heads, latent), bf16),
            in_specs=[vmem] * 3,
            out_specs=hbm,
            scratch_shapes=[pltpu.VMEM((heads, latent), bf16), dma((2,))],
            compiler_params=pltpu.CompilerParams(vmem_limit_bytes=VMEM_BYTES),
        )(done, part, drecv)

    return jax.shard_map(
        local_step, mesh=mesh,
        in_specs=(P('dp', 'dcp', None), P('dp', None, 'dcp', None, None), P('dp')),
        out_specs=P(('dp', 'dcp'), None, None), check_vma=False)
```

```python
import functools

import jax
import jax.numpy as jnp
from jax import lax
from jax.experimental import pallas as pl
from jax.experimental.pallas import tpu as pltpu
from jax.sharding import PartitionSpec as P

ROPE_DIM = 64
QK_DIM = 192
CORES = 2
SLOTS = 4
AHEAD = 3
REUSE = 6
LANES = 128
VMEM_BYTES = 36 * 2**20
F32 = jnp.float32


def columns(row):
    return jnp.transpose(jnp.broadcast_to(row, (row.shape[1], row.shape[1])))


def weights(*lses):
    top = functools.reduce(jnp.maximum, lses)
    exps = [jnp.exp(one - top) for one in lses]
    total = functools.reduce(jnp.add, exps)
    return [columns(one / total) for one in exps], top + jnp.log(total)


def finish(local, received, out_ref):
    heads, latent = out_ref.shape
    blocks = latent // LANES // 2
    lse_row = pl.ds(blocks * heads, 1)
    for h in range(2):
        parts = [local.at[h], received.at[0, h], received.at[1, h]]
        cols, _ = weights(*(one[lse_row] for one in parts))
        for i in range(blocks):
            rows = pl.ds(i * heads, heads)
            total = functools.reduce(jnp.add, [col * one[rows] for col, one in zip(cols, parts)])
            out_ref[:, pl.ds((h * blocks + i) * LANES, LANES)] = total.astype(jnp.bfloat16)


def kernel(
    group, len_hbm, q_hbm, c_hbm, out_ref, part, drecv,
    len_ref, rope, qbuf, cbuf, osend, lsend, orecv, lrecv, own, lown, frecv,
    lensem, csem, qsem, ag_send, ag_recv, sib_q, sib_send, sib_recv, ring_send, f_recv, d_recv,
):
    rounds, _, tiles, own_heads, lanes = qbuf.shape
    chips = group // CORES
    steps = rounds * chips
    seqs = steps * CORES
    heads, latent = osend.shape[1:]
    blocks = latent // lanes // 2
    lse_row = pl.ds(blocks * heads, 1)
    rows = pl.ds(0, blocks * heads + 1)

    def block_rows(i):
        return pl.ds(i * heads, heads)
    pages, width, page_len = cbuf.shape[1:]
    me = lax.axis_index('dcp')
    chip, core = me // CORES, me % CORES
    sibling = chip * CORES + 1 - core
    right = ((chip + 1) % chips) * CORES + core
    left = ((chip + chips - 1) % chips) * CORES + core
    far = ((chip + 2) % chips) * CORES + core

    def remote(src, dst, send, recv, target):
        return pltpu.make_async_remote_copy(
            src_ref=src, dst_ref=dst, send_sem=send, recv_sem=recv,
            device_id={'dcp': target}, device_id_type=pl.DeviceIdType.MESH)

    def wait_bytes(ref, sem):
        pltpu.make_async_copy(ref, ref, sem).wait()

    def place(n, other):
        r, k = n // chips, n % chips
        dest_chip = (chip + 2 - k + chips) % chips
        dest_core = (1 - core) if other else core
        return r, dest_chip * CORES + dest_core

    def fetch(n, e):
        r, d = place(n, e == 0)
        slot = (2 * n + e) % SLOTS
        return pltpu.make_async_copy(c_hbm.at[d, r, :, 0], cbuf.at[slot], csem.at[slot])

    latent_tiles = group * latent // lanes

    def q_load():
        yield pltpu.make_async_copy(q_hbm.at[:, 0, :, latent:], rope.at[:, 0], qsem.at[2])
        for r in range(rounds):
            for c in range(latent // lanes):
                yield pltpu.make_async_copy(
                    q_hbm.at[:, r, :, c * lanes : (c + 1) * lanes], qbuf.at[r, me, c * group : (c + 1) * group],
                    qsem.at[min(r, 1)])
            if r == 0:
                yield pltpu.make_async_copy(q_hbm.at[:, 1:, :, latent:], rope.at[:, 1:], qsem.at[3])

    def q_pack(r):
        for p in range(group // 2):
            qbuf[r, me, latent_tiles + p] = jnp.concatenate([rope[2 * p, r], rope[2 * p + 1, r]], axis=1)

    def q_sem(r, kind):
        return sib_q.at[r] if kind == 2 else ag_recv.at[r % REUSE, kind]

    def q_copy(r, kind, block, target):
        return remote(qbuf.at[r, block], qbuf.at[r, block], ag_send, q_sem(r, kind), target)

    def q_wait(r, kind, count):
        wait_bytes(qbuf.at[r, 0:count], q_sem(r, kind))

    def q_first(r):
        q_copy(r, 0, me, right).start()
        q_copy(r, 0, me, left).start()
        q_copy(r, 2, me, sibling).start()

    def q_second(r):
        q_wait(r, 0, 2)

        @pl.when(r % 2 == 0)
        def _():
            q_copy(r, 1, left, right).start()

        @pl.when(r % 2 == 1)
        def _():
            q_copy(r, 1, right, left).start()

        q_copy(r, 2, left, sibling).start()
        q_copy(r, 2, right, sibling).start()

    def q_third(r):
        q_wait(r, 1, 1)
        q_copy(r, 2, far, sibling).start()

    def q_last(r):
        q_wait(r, 2, chips)

    def attend(n, e):
        r, d = place(n, e == 0)
        slot = (2 * n + e) % SLOTS
        fetch(n, e).wait()
        nxt = 2 * n + e + SLOTS - 1

        @pl.when(nxt < seqs)
        def _():
            fetch((2 * n + e + SLOTS - 1) // 2, (e + SLOTS - 1) % 2).start()

        q = [qbuf[r, :, c * group + d].reshape(heads, lanes) for c in range(latent // lanes)]
        pair = qbuf[r, :, latent_tiles + d // 2].reshape(heads, lanes)
        q.append(jnp.where(d % 2 == 0, pair[:, : lanes // 2], pair[:, lanes // 2 :]))
        q = jnp.concatenate(q, axis=1)
        length = len_ref[d * rounds + r]
        scores = []
        for j in range(pages):
            s = jnp.dot(q, cbuf[slot, j], preferred_element_type=F32) * (QK_DIM ** -0.5)
            pos = lax.broadcasted_iota(jnp.int32, s.shape, 1) + (j * group + me) * page_len
            scores.append(jnp.where(pos < length, s, -1e30))
        top = functools.reduce(jnp.maximum, [jnp.max(s, axis=1, keepdims=True) for s in scores])
        exps = [jnp.exp(s - top) for s in scores]
        total = functools.reduce(jnp.add, [jnp.sum(w, axis=1, keepdims=True) for w in exps])
        acc = functools.reduce(jnp.add, [
            lax.dot_general(w.astype(jnp.bfloat16), cbuf[slot, j, :latent], (((1,), (1,)), ((), ())),
                            preferred_element_type=F32)
            for j, w in enumerate(exps)])
        lse = top + jnp.log(total)
        lse = jnp.transpose(jnp.broadcast_to(lse, (heads, heads)))[0:1]
        return (acc / total).astype(jnp.bfloat16), lse

    def sib_o(n):
        return remote(osend.at[n], orecv.at[n], sib_send.at[0], sib_recv.at[n % 4, 0], sibling)

    def sib_l(n):
        return remote(lsend.at[n], lrecv.at[n], sib_send.at[1], sib_recv.at[n % 4, 1], sibling)

    def ring(r, kind):
        target = right if kind % 2 == 0 else left
        k = (0, 0, 1, 3, 1, 3)[kind]
        h = (0, 1, 1, 0, 0, 1)[kind]
        if kind < 2:
            dst, sem = frecv.at[r, h, rows], f_recv.at[r % 4, h]
        else:
            dst, sem = drecv.at[r, kind % 2, h, rows], d_recv.at[(r + 1) // rounds]
        return remote(part.at[r, k, h, rows], dst, ring_send, sem, target)

    def merge(n):
        r, k = n // chips, n % chips
        sib_o(n).wait_recv()
        sib_l(n).wait_recv()
        slot = n % 2
        (wa, wb), lse = weights(lown[slot], lrecv[n])
        for h in range(2):
            for i in range(blocks):
                cols = pl.ds((h * blocks + i) * lanes, lanes)
                part[r, k, h, block_rows(i)] = wa * own[slot, :, cols].astype(F32) + wb * orecv[n, :, cols].astype(F32)
            part[r, k, h, lse_row] = lse

        @pl.when(k == 0)
        def _():
            ring(r, 0).start()
            ring(r, 1).start()

        @pl.when(k == 1)
        def _():
            ring(r, 2).start()

        @pl.when(k == 3)
        def _():
            ring(r, 3).start()

    def relay(r):
        for kind in (4, 5):
            h = kind % 2
            k = (1, 3)[h]
            ring(r, h).wait_recv()
            (wa, wb), lse = weights(part[r, k, h, lse_row], frecv[r, h, lse_row])
            for i in range(blocks):
                part[r, k, h, block_rows(i)] = wa * part[r, k, h, block_rows(i)] + wb * frecv[r, h, block_rows(i)]
            part[r, k, h, lse_row] = lse
            ring(r, kind).start()

    barrier = pltpu.get_barrier_semaphore()
    for neighbour in (left, right, sibling):
        pl.semaphore_signal(barrier, inc=1, device_id={'dcp': neighbour}, device_id_type=pl.DeviceIdType.MESH)
    for copy in q_load():
        copy.start()
    len_copy = pltpu.make_async_copy(len_hbm, len_ref, lensem)
    len_copy.start()
    for u in range(SLOTS - 1):
        fetch(u // 2, u % 2).start()
    pl.semaphore_wait(barrier, 3)
    for c in range(latent // lanes):
        to = pl.ds(c * group, group)
        for target in (right, left):
            remote(q_hbm.at[:, 0, :, c * lanes : (c + 1) * lanes], qbuf.at[0, me, to], ag_send, ag_recv.at[0, 0], target).start()
    wait_bytes(rope.at[:, 0], qsem.at[2])
    q_pack(0)
    to = pl.ds(latent_tiles, group // 2)
    for target in (right, left):
        remote(qbuf.at[0, me, to], qbuf.at[0, me, to], ag_send, ag_recv.at[0, 0], target).start()
    wait_bytes(qbuf.at[0, me, 0:latent_tiles], qsem.at[0])
    q_copy(0, 2, me, sibling).start()
    wait_bytes(rope.at[:, 1:], qsem.at[3])
    for r in range(1, rounds):
        q_pack(r)
    wait_bytes(qbuf.at[1:rounds, me, 0:latent_tiles], qsem.at[1])
    for r in range(1, AHEAD):
        q_first(r)
    len_copy.wait()
    q_second(0)
    q_first(AHEAD)
    q_second(1)
    q_first(AHEAD + 1)
    q_third(0)

    @pl.loop(0, rounds)
    def _(r):
        @pl.when(r + 2 < rounds)
        def _():
            q_second(r + 2)

        @pl.when(r + AHEAD + 2 < rounds)
        def _():
            q_first(r + AHEAD + 2)

        @pl.when(r + 1 < rounds)
        def _():
            q_third(r + 1)

        q_last(r)

        @pl.loop(0, chips)
        def _(k):
            n = r * chips + k
            o, lse = attend(n, 0)
            osend[n] = o
            lsend[n] = lse
            sib_o(n).start()
            sib_l(n).start()
            o, lse = attend(n, 1)
            own[n % 2] = o
            lown[n % 2] = lse

            @pl.when(n >= 1)
            def _():
                merge(n - 1)

        @pl.when(r >= 1)
        def _():
            relay(r - 1)

    merge(steps - 1)
    relay(rounds - 1)

    wait_bytes(drecv.at[0 : rounds - 1, :, :, rows], d_recv.at[0])

    @pl.loop(0, rounds - 1)
    def _(r):
        finish(part.at[r, 2], drecv.at[r], out_ref.at[r])

    wait_bytes(drecv.at[rounds - 1, :, :, rows], d_recv.at[1])

    wait_bytes(qbuf.at[:, 0:7], ag_send)
    wait_bytes(osend, sib_send.at[0])
    wait_bytes(lsend, sib_send.at[1])
    wait_bytes(part.at[:, 0:3, :, rows], ring_send)


def put_out(done, part, drecv, out_hbm, last, sems):
    n = done.shape[0]
    copies = [
        pltpu.make_async_copy(done, out_hbm.at[pl.ds(0, n)], sems.at[0]),
        pltpu.make_async_copy(last, out_hbm.at[n], sems.at[1]),
    ]
    copies[0].start()
    finish(part.at[n, 2], drecv.at[n], last)
    copies[1].start()
    for copy in copies:
        copy.wait()


def solution(mesh):
    group = mesh.shape['dcp']
    chips = group // CORES

    def local_step(q_blk, cache_blk, len_blk):
        batch, own_heads, width = q_blk.shape
        pages, page_len = cache_blk.shape[1], cache_blk.shape[3]
        latent = width - ROPE_DIM
        rounds = batch // group
        heads = own_heads * group
        steps = rounds * chips
        rows = latent // LANES // 2 * heads + 8
        q = q_blk.reshape(group, rounds, own_heads, width)
        cache = jnp.swapaxes(cache_blk, 3, 4).reshape(group, rounds, pages, 1, width, page_len)
        bf16 = jnp.bfloat16
        dma = pltpu.SemaphoreType.DMA
        tiles = group * latent // LANES + group // 2
        hbm = pl.BlockSpec(memory_space=pltpu.HBM)
        vmem = pl.BlockSpec(memory_space=pltpu.VMEM)
        done, part, drecv = pl.pallas_call(
            functools.partial(kernel, group),
            out_shape=[
                jax.ShapeDtypeStruct((rounds - 1, heads, latent), bf16),
                jax.ShapeDtypeStruct((rounds, chips, 2, rows, LANES), F32),
                jax.ShapeDtypeStruct((rounds, 2, 2, rows, LANES), F32),
            ],
            in_specs=[hbm, hbm, hbm],
            out_specs=[vmem] * 3,
            scratch_shapes=[
                pltpu.SMEM((batch,), jnp.int32),
                pltpu.VMEM((group, rounds, own_heads, ROPE_DIM), bf16),
                pltpu.VMEM((rounds, group, tiles, own_heads, LANES), bf16),
                pltpu.VMEM((SLOTS, pages, width, page_len), bf16),
                pltpu.VMEM((steps, heads, latent), bf16),
                pltpu.VMEM((steps, 1, heads), F32),
                pltpu.VMEM((steps, heads, latent), bf16),
                pltpu.VMEM((steps, 1, heads), F32),
                pltpu.VMEM((2, heads, latent), bf16),
                pltpu.VMEM((2, 1, heads), F32),
                pltpu.VMEM((rounds, 2, rows, LANES), F32),
                dma,
                dma((SLOTS,)),
                dma((4,)),
                dma,
                dma((REUSE, 2)),
                dma((rounds,)),
                dma((2,)),
                dma((4, 2)),
                dma,
                dma((4, 2)),
                dma((2,)),
            ],
            compiler_params=pltpu.CompilerParams(
                collective_id=0, has_side_effects=True, vmem_limit_bytes=VMEM_BYTES),
        )(*(pltpu.with_memory_space_constraint(x, pltpu.HBM) for x in (len_blk, q, cache)))
        return pl.pallas_call(
            put_out,
            out_shape=jax.ShapeDtypeStruct((rounds, heads, latent), bf16),
            in_specs=[vmem] * 3,
            out_specs=hbm,
            scratch_shapes=[pltpu.VMEM((heads, latent), bf16), dma((2,))],
            compiler_params=pltpu.CompilerParams(vmem_limit_bytes=VMEM_BYTES),
        )(done, part, drecv)

    return jax.shard_map(
        local_step, mesh=mesh,
        in_specs=(P('dp', 'dcp', None), P('dp', None, 'dcp', None, None), P('dp')),
        out_specs=P(('dp', 'dcp'), None, None), check_vma=False)
```

```python
import functools

import jax
import jax.numpy as jnp
from jax import lax
from jax.experimental import pallas as pl
from jax.experimental.pallas import tpu as pltpu
from jax.sharding import PartitionSpec as P

ROPE_DIM = 64
QK_DIM = 192
CORES = 2
SLOTS = 4
AHEAD = 3
REUSE = 6
LANES = 128
VMEM_BYTES = 36 * 2**20
F32 = jnp.float32


def columns(row):
    return jnp.transpose(jnp.broadcast_to(row, (row.shape[1], row.shape[1])))


def weights(*lses):
    top = functools.reduce(jnp.maximum, lses)
    exps = [jnp.exp(one - top) for one in lses]
    total = functools.reduce(jnp.add, exps)
    return [columns(one / total) for one in exps], top + jnp.log(total)


def finish(local, received, out_ref):
    heads, latent = out_ref.shape
    blocks = latent // LANES // 2
    lse_row = pl.ds(blocks * heads, 1)
    for h in range(2):
        parts = [local.at[h], received.at[0, h], received.at[1, h]]
        cols, _ = weights(*(one[lse_row] for one in parts))
        for i in range(blocks):
            rows = pl.ds(i * heads, heads)
            total = functools.reduce(jnp.add, [col * one[rows] for col, one in zip(cols, parts)])
            out_ref[:, pl.ds((h * blocks + i) * LANES, LANES)] = total.astype(jnp.bfloat16)


def kernel(
    group, len_hbm, q_hbm, c_hbm, out_ref, part, drecv,
    len_ref, rope, qbuf, cbuf, osend, lsend, orecv, lrecv, own, lown, frecv,
    lensem, csem, qsem, ag_send, ag_recv, sib_q, sib_send, sib_recv, ring_send, f_recv, d_recv,
):
    rounds, _, tiles, own_heads, lanes = qbuf.shape
    chips = group // CORES
    steps = rounds * chips
    seqs = steps * CORES
    heads, latent = osend.shape[1:]
    blocks = latent // lanes // 2
    lse_row = pl.ds(blocks * heads, 1)
    rows = pl.ds(0, blocks * heads + 1)

    def block_rows(i):
        return pl.ds(i * heads, heads)
    pages, width, page_len = cbuf.shape[1:]
    me = lax.axis_index('dcp')
    chip, core = me // CORES, me % CORES
    sibling = chip * CORES + 1 - core
    right = ((chip + 1) % chips) * CORES + core
    left = ((chip + chips - 1) % chips) * CORES + core
    far = ((chip + 2) % chips) * CORES + core

    def remote(src, dst, send, recv, target):
        return pltpu.make_async_remote_copy(
            src_ref=src, dst_ref=dst, send_sem=send, recv_sem=recv,
            device_id={'dcp': target}, device_id_type=pl.DeviceIdType.MESH)

    def wait_bytes(ref, sem):
        pltpu.make_async_copy(ref, ref, sem).wait()

    def place(n, other):
        r, k = n // chips, n % chips
        dest_chip = (chip + 2 - k + chips) % chips
        dest_core = (1 - core) if other else core
        return r, dest_chip * CORES + dest_core

    def fetch(n, e):
        r, d = place(n, e == 0)
        slot = (2 * n + e) % SLOTS
        return pltpu.make_async_copy(c_hbm.at[d, r, :, 0], cbuf.at[slot], csem.at[slot])

    latent_tiles = group * latent // lanes

    def q_load():
        yield pltpu.make_async_copy(q_hbm.at[:, 0, :, latent:], rope.at[:, 0], qsem.at[2])
        for r in range(rounds):
            for c in range(latent // lanes):
                yield pltpu.make_async_copy(
                    q_hbm.at[:, r, :, c * lanes : (c + 1) * lanes], qbuf.at[r, me, c * group : (c + 1) * group],
                    qsem.at[min(r, 1)])
            if r == 0:
                yield pltpu.make_async_copy(q_hbm.at[:, 1:, :, latent:], rope.at[:, 1:], qsem.at[3])

    def q_pack(r):
        for p in range(group // 2):
            qbuf[r, me, latent_tiles + p] = jnp.concatenate([rope[2 * p, r], rope[2 * p + 1, r]], axis=1)

    def q_sem(r, kind):
        return sib_q.at[r] if kind == 2 else ag_recv.at[r % REUSE, kind]

    def q_copy(r, kind, block, target):
        return remote(qbuf.at[r, block], qbuf.at[r, block], ag_send, q_sem(r, kind), target)

    def q_wait(r, kind, count):
        wait_bytes(qbuf.at[r, 0:count], q_sem(r, kind))

    def q_first(r):
        q_copy(r, 0, me, right).start()
        q_copy(r, 0, me, left).start()
        q_copy(r, 2, me, sibling).start()

    def q_second(r):
        q_wait(r, 0, 2)

        @pl.when(r % 2 == 0)
        def _():
            q_copy(r, 1, left, right).start()

        @pl.when(r % 2 == 1)
        def _():
            q_copy(r, 1, right, left).start()

        q_copy(r, 2, left, sibling).start()
        q_copy(r, 2, right, sibling).start()

    def q_third(r):
        q_wait(r, 1, 1)
        q_copy(r, 2, far, sibling).start()

    def q_last(r):
        q_wait(r, 2, chips)

    def attend(n, e):
        r, d = place(n, e == 0)
        slot = (2 * n + e) % SLOTS
        fetch(n, e).wait()
        nxt = 2 * n + e + SLOTS - 1

        @pl.when(nxt < seqs)
        def _():
            fetch((2 * n + e + SLOTS - 1) // 2, (e + SLOTS - 1) % 2).start()

        q = [qbuf[r, :, c * group + d].reshape(heads, lanes) for c in range(latent // lanes)]
        pair = qbuf[r, :, latent_tiles + d // 2].reshape(heads, lanes)
        q.append(jnp.where(d % 2 == 0, pair[:, : lanes // 2], pair[:, lanes // 2 :]))
        q = jnp.concatenate(q, axis=1)
        length = len_ref[d * rounds + r]
        scores = []
        for j in range(pages):
            s = jnp.dot(q, cbuf[slot, j], preferred_element_type=F32) * (QK_DIM ** -0.5)
            pos = lax.broadcasted_iota(jnp.int32, s.shape, 1) + (j * group + me) * page_len
            scores.append(jnp.where(pos < length, s, -1e30))
        top = functools.reduce(jnp.maximum, [jnp.max(s, axis=1, keepdims=True) for s in scores])
        exps = [jnp.exp(s - top) for s in scores]
        total = functools.reduce(jnp.add, [jnp.sum(w, axis=1, keepdims=True) for w in exps])
        acc = functools.reduce(jnp.add, [
            lax.dot_general(w.astype(jnp.bfloat16), cbuf[slot, j, :latent], (((1,), (1,)), ((), ())),
                            preferred_element_type=F32)
            for j, w in enumerate(exps)])
        lse = top + jnp.log(total)
        lse = jnp.transpose(jnp.broadcast_to(lse, (heads, heads)))[0:1]
        return (acc / total).astype(jnp.bfloat16), lse

    def sib_o(n):
        return remote(osend.at[n], orecv.at[n], sib_send.at[0], sib_recv.at[n % 4, 0], sibling)

    def sib_l(n):
        return remote(lsend.at[n], lrecv.at[n], sib_send.at[1], sib_recv.at[n % 4, 1], sibling)

    def ring(r, kind):
        target = right if kind % 2 == 0 else left
        k = (0, 0, 1, 3, 1, 3)[kind]
        h = (0, 1, 1, 0, 0, 1)[kind]
        if kind < 2:
            dst, sem = frecv.at[r, h, rows], f_recv.at[r % 4, h]
        else:
            dst, sem = drecv.at[r, kind % 2, h, rows], d_recv.at[(r + 1) // rounds]
        return remote(part.at[r, k, h, rows], dst, ring_send, sem, target)

    def merge(n):
        r, k = n // chips, n % chips
        sib_o(n).wait_recv()
        sib_l(n).wait_recv()
        slot = n % 2
        (wa, wb), lse = weights(lown[slot], lrecv[n])
        for h in range(2):
            for i in range(blocks):
                cols = pl.ds((h * blocks + i) * lanes, lanes)
                part[r, k, h, block_rows(i)] = wa * own[slot, :, cols].astype(F32) + wb * orecv[n, :, cols].astype(F32)
            part[r, k, h, lse_row] = lse

        @pl.when(k == 0)
        def _():
            ring(r, 0).start()
            ring(r, 1).start()

        @pl.when(k == 1)
        def _():
            ring(r, 2).start()

        @pl.when(k == 3)
        def _():
            ring(r, 3).start()

    def relay(r):
        for kind in (4, 5):
            h = kind % 2
            k = (1, 3)[h]
            ring(r, h).wait_recv()
            (wa, wb), lse = weights(part[r, k, h, lse_row], frecv[r, h, lse_row])
            for i in range(blocks):
                part[r, k, h, block_rows(i)] = wa * part[r, k, h, block_rows(i)] + wb * frecv[r, h, block_rows(i)]
            part[r, k, h, lse_row] = lse
            ring(r, kind).start()

    barrier = pltpu.get_barrier_semaphore()
    for neighbour in (left, right, sibling):
        pl.semaphore_signal(barrier, inc=1, device_id={'dcp': neighbour}, device_id_type=pl.DeviceIdType.MESH)
    for copy in q_load():
        copy.start()
    len_copy = pltpu.make_async_copy(len_hbm, len_ref, lensem)
    len_copy.start()
    for u in range(SLOTS - 1):
        fetch(u // 2, u % 2).start()
    pl.semaphore_wait(barrier, 3)
    for c in range(latent // lanes):
        to = pl.ds(c * group, group)
        for target in (right, left):
            remote(q_hbm.at[:, 0, :, c * lanes : (c + 1) * lanes], qbuf.at[0, me, to], ag_send, ag_recv.at[0, 0], target).start()
    wait_bytes(rope.at[:, 0], qsem.at[2])
    q_pack(0)
    to = pl.ds(latent_tiles, group // 2)
    for target in (right, left):
        remote(qbuf.at[0, me, to], qbuf.at[0, me, to], ag_send, ag_recv.at[0, 0], target).start()
    wait_bytes(qbuf.at[0, me, 0:latent_tiles], qsem.at[0])
    q_copy(0, 2, me, sibling).start()
    wait_bytes(rope.at[:, 1:], qsem.at[3])
    for r in range(1, rounds):
        q_pack(r)
    wait_bytes(qbuf.at[1:rounds, me, 0:latent_tiles], qsem.at[1])
    q_first(1)
    len_copy.wait()
    q_second(0)
    q_first(2)
    q_first(3)
    q_second(1)
    q_first(4)
    q_third(0)

    @pl.loop(0, rounds)
    def _(r):
        @pl.when(r + 2 < rounds)
        def _():
            q_second(r + 2)

        @pl.when(r + AHEAD + 2 < rounds)
        def _():
            q_first(r + AHEAD + 2)

        q_last(r)

        @pl.loop(0, chips)
        def _(k):
            n = r * chips + k

            @pl.when(jnp.logical_and(k == 2, r + 1 < rounds))
            def _():
                q_third(r + 1)

            o, lse = attend(n, 0)
            osend[n] = o
            lsend[n] = lse
            sib_o(n).start()
            sib_l(n).start()
            o, lse = attend(n, 1)
            own[n % 2] = o
            lown[n % 2] = lse

            @pl.when(n >= 1)
            def _():
                merge(n - 1)

        @pl.when(r >= 1)
        def _():
            relay(r - 1)

    merge(steps - 1)
    relay(rounds - 1)

    wait_bytes(drecv.at[0 : rounds - 1, :, :, rows], d_recv.at[0])

    @pl.loop(0, rounds - 1)
    def _(r):
        finish(part.at[r, 2], drecv.at[r], out_ref.at[r])

    wait_bytes(drecv.at[rounds - 1, :, :, rows], d_recv.at[1])

    wait_bytes(qbuf.at[:, 0:7], ag_send)
    wait_bytes(osend, sib_send.at[0])
    wait_bytes(lsend, sib_send.at[1])
    wait_bytes(part.at[:, 0:3, :, rows], ring_send)


def put_out(done, part, drecv, out_hbm, last, sems):
    n = done.shape[0]
    copies = [
        pltpu.make_async_copy(done, out_hbm.at[pl.ds(0, n)], sems.at[0]),
        pltpu.make_async_copy(last, out_hbm.at[n], sems.at[1]),
    ]
    copies[0].start()
    finish(part.at[n, 2], drecv.at[n], last)
    copies[1].start()
    for copy in copies:
        copy.wait()


def solution(mesh):
    group = mesh.shape['dcp']
    chips = group // CORES

    def local_step(q_blk, cache_blk, len_blk):
        batch, own_heads, width = q_blk.shape
        pages, page_len = cache_blk.shape[1], cache_blk.shape[3]
        latent = width - ROPE_DIM
        rounds = batch // group
        heads = own_heads * group
        steps = rounds * chips
        rows = latent // LANES // 2 * heads + 8
        q = q_blk.reshape(group, rounds, own_heads, width)
        cache = jnp.swapaxes(cache_blk, 3, 4).reshape(group, rounds, pages, 1, width, page_len)
        bf16 = jnp.bfloat16
        dma = pltpu.SemaphoreType.DMA
        tiles = group * latent // LANES + group // 2
        hbm = pl.BlockSpec(memory_space=pltpu.HBM)
        vmem = pl.BlockSpec(memory_space=pltpu.VMEM)
        done, part, drecv = pl.pallas_call(
            functools.partial(kernel, group),
            out_shape=[
                jax.ShapeDtypeStruct((rounds - 1, heads, latent), bf16),
                jax.ShapeDtypeStruct((rounds, chips, 2, rows, LANES), F32),
                jax.ShapeDtypeStruct((rounds, 2, 2, rows, LANES), F32),
            ],
            in_specs=[hbm, hbm, hbm],
            out_specs=[vmem] * 3,
            scratch_shapes=[
                pltpu.SMEM((batch,), jnp.int32),
                pltpu.VMEM((group, rounds, own_heads, ROPE_DIM), bf16),
                pltpu.VMEM((rounds, group, tiles, own_heads, LANES), bf16),
                pltpu.VMEM((SLOTS, pages, width, page_len), bf16),
                pltpu.VMEM((steps, heads, latent), bf16),
                pltpu.VMEM((steps, 1, heads), F32),
                pltpu.VMEM((steps, heads, latent), bf16),
                pltpu.VMEM((steps, 1, heads), F32),
                pltpu.VMEM((2, heads, latent), bf16),
                pltpu.VMEM((2, 1, heads), F32),
                pltpu.VMEM((rounds, 2, rows, LANES), F32),
                dma,
                dma((SLOTS,)),
                dma((4,)),
                dma,
                dma((REUSE, 2)),
                dma((rounds,)),
                dma((2,)),
                dma((4, 2)),
                dma,
                dma((4, 2)),
                dma((2,)),
            ],
            compiler_params=pltpu.CompilerParams(
                collective_id=0, has_side_effects=True, vmem_limit_bytes=VMEM_BYTES),
        )(*(pltpu.with_memory_space_constraint(x, pltpu.HBM) for x in (len_blk, q, cache)))
        return pl.pallas_call(
            put_out,
            out_shape=jax.ShapeDtypeStruct((rounds, heads, latent), bf16),
            in_specs=[vmem] * 3,
            out_specs=hbm,
            scratch_shapes=[pltpu.VMEM((heads, latent), bf16), dma((2,))],
            compiler_params=pltpu.CompilerParams(vmem_limit_bytes=VMEM_BYTES),
        )(done, part, drecv)

    return jax.shard_map(
        local_step, mesh=mesh,
        in_specs=(P('dp', 'dcp', None), P('dp', None, 'dcp', None, None), P('dp')),
        out_specs=P(('dp', 'dcp'), None, None), check_vma=False)
```

```python
import functools

import jax
import jax.numpy as jnp
from jax import lax
from jax.experimental import pallas as pl
from jax.experimental.pallas import tpu as pltpu
from jax.sharding import PartitionSpec as P

ROPE_DIM = 64
QK_DIM = 192
CORES = 2
SLOTS = 3
AHEAD = 3
REUSE = 6
LANES = 128
VMEM_BYTES = 36 * 2**20
F32 = jnp.float32


def columns(row):
    return jnp.transpose(jnp.broadcast_to(row, (row.shape[1], row.shape[1])))


def weights(*lses):
    top = functools.reduce(jnp.maximum, lses)
    exps = [jnp.exp(one - top) for one in lses]
    total = functools.reduce(jnp.add, exps)
    return [columns(one / total) for one in exps], top + jnp.log(total)


def finish(local, received, out_ref):
    heads, latent = out_ref.shape
    blocks = latent // LANES // 2
    lse_row = pl.ds(blocks * heads, 1)
    for h in range(2):
        parts = [local.at[h], received.at[0, h], received.at[1, h]]
        cols, _ = weights(*(one[lse_row] for one in parts))
        for i in range(blocks):
            rows = pl.ds(i * heads, heads)
            total = functools.reduce(jnp.add, [col * one[rows] for col, one in zip(cols, parts)])
            out_ref[:, pl.ds((h * blocks + i) * LANES, LANES)] = total.astype(jnp.bfloat16)


def kernel(
    group, len_hbm, q_hbm, c_hbm, out_ref, part, drecv,
    len_ref, rope, qbuf, cbuf, osend, lsend, orecv, lrecv, own, lown, frecv,
    lensem, csem, qsem, ag_send, ag_recv, sib_q, sib_send, sib_recv, ring_send, f_recv, d_recv,
):
    rounds, _, tiles, own_heads, lanes = qbuf.shape
    chips = group // CORES
    steps = rounds * chips
    seqs = steps * CORES
    heads, latent = osend.shape[1:]
    blocks = latent // lanes // 2
    lse_row = pl.ds(blocks * heads, 1)
    rows = pl.ds(0, blocks * heads + 1)

    def block_rows(i):
        return pl.ds(i * heads, heads)
    pages, width, page_len = cbuf.shape[1:]
    me = lax.axis_index('dcp')
    chip, core = me // CORES, me % CORES
    sibling = chip * CORES + 1 - core
    right = ((chip + 1) % chips) * CORES + core
    left = ((chip + chips - 1) % chips) * CORES + core
    far = ((chip + 2) % chips) * CORES + core

    def remote(src, dst, send, recv, target):
        return pltpu.make_async_remote_copy(
            src_ref=src, dst_ref=dst, send_sem=send, recv_sem=recv,
            device_id={'dcp': target}, device_id_type=pl.DeviceIdType.MESH)

    def wait_bytes(ref, sem):
        pltpu.make_async_copy(ref, ref, sem).wait()

    def place(n, other):
        r, k = n // chips, n % chips
        dest_chip = (chip + 2 - k + chips) % chips
        dest_core = (1 - core) if other else core
        return r, dest_chip * CORES + dest_core

    def fetch(n, e):
        r, d = place(n, e == 0)
        slot = (2 * n + e) % SLOTS
        return pltpu.make_async_copy(c_hbm.at[d, r, :, 0], cbuf.at[slot], csem.at[slot])

    latent_tiles = group * latent // lanes

    def q_load():
        yield pltpu.make_async_copy(q_hbm.at[:, 0, :, latent:], rope.at[:, 0], qsem.at[2])
        for r in range(rounds):
            for c in range(latent // lanes):
                yield pltpu.make_async_copy(
                    q_hbm.at[:, r, :, c * lanes : (c + 1) * lanes], qbuf.at[r, me, c * group : (c + 1) * group],
                    qsem.at[min(r, 1)])
            if r == 0:
                yield pltpu.make_async_copy(q_hbm.at[:, 1:, :, latent:], rope.at[:, 1:], qsem.at[3])

    def q_pack(r):
        for p in range(group // 2):
            qbuf[r, me, latent_tiles + p] = jnp.concatenate([rope[2 * p, r], rope[2 * p + 1, r]], axis=1)

    def q_sem(r, kind):
        return sib_q.at[r % REUSE] if kind == 2 else ag_recv.at[r % REUSE, kind]

    def q_copy(r, kind, block, target):
        return remote(qbuf.at[r, block], qbuf.at[r, block], ag_send, q_sem(r, kind), target)

    def q_wait(r, kind, count):
        wait_bytes(qbuf.at[r, 0:count], q_sem(r, kind))

    def q_first(r):
        q_copy(r, 0, me, right).start()
        q_copy(r, 0, me, left).start()
        q_copy(r, 2, me, sibling).start()

    def q_second(r):
        q_wait(r, 0, 2)

        @pl.when(r % 2 == 0)
        def _():
            q_copy(r, 1, left, right).start()

        @pl.when(r % 2 == 1)
        def _():
            q_copy(r, 1, right, left).start()

        q_copy(r, 2, left, sibling).start()
        q_copy(r, 2, right, sibling).start()

    def q_third(r):
        q_wait(r, 1, 1)
        q_copy(r, 2, far, sibling).start()

    def q_last(r):
        q_wait(r, 2, chips)

    def attend(n, e):
        r, d = place(n, e == 0)
        slot = (2 * n + e) % SLOTS
        fetch(n, e).wait()
        nxt = 2 * n + e + SLOTS - 1

        @pl.when(nxt < seqs)
        def _():
            fetch((2 * n + e + SLOTS - 1) // 2, (e + SLOTS - 1) % 2).start()

        q = [qbuf[r, :, c * group + d].reshape(heads, lanes) for c in range(latent // lanes)]
        pair = qbuf[r, :, latent_tiles + d // 2].reshape(heads, lanes)
        q.append(jnp.where(d % 2 == 0, pair[:, : lanes // 2], pair[:, lanes // 2 :]))
        q = jnp.concatenate(q, axis=1)
        length = len_ref[d * rounds + r]
        scores = []
        for j in range(pages):
            s = jnp.dot(q, cbuf[slot, j], preferred_element_type=F32) * (QK_DIM ** -0.5)
            pos = lax.broadcasted_iota(jnp.int32, s.shape, 1) + (j * group + me) * page_len
            scores.append(jnp.where(pos < length, s, -1e30))
        top = functools.reduce(jnp.maximum, [jnp.max(s, axis=1, keepdims=True) for s in scores])
        exps = [jnp.exp(s - top) for s in scores]
        total = functools.reduce(jnp.add, [jnp.sum(w, axis=1, keepdims=True) for w in exps])
        acc = functools.reduce(jnp.add, [
            lax.dot_general(w.astype(jnp.bfloat16), cbuf[slot, j, :latent], (((1,), (1,)), ((), ())),
                            preferred_element_type=F32)
            for j, w in enumerate(exps)])
        lse = top + jnp.log(total)
        lse = jnp.transpose(jnp.broadcast_to(lse, (heads, heads)))[0:1]
        return (acc / total).astype(jnp.bfloat16), lse

    def sib_o(n):
        return remote(osend.at[n], orecv.at[n], sib_send.at[0], sib_recv.at[n % 4, 0], sibling)

    def sib_l(n):
        return remote(lsend.at[n], lrecv.at[n], sib_send.at[1], sib_recv.at[n % 4, 1], sibling)

    def ring(r, kind):
        target = right if kind % 2 == 0 else left
        k = (0, 0, 1, 3, 1, 3)[kind]
        h = (0, 1, 1, 0, 0, 1)[kind]
        if kind < 2:
            dst, sem = frecv.at[r, h, rows], f_recv.at[r % 4]
        else:
            dst, sem = drecv.at[r, kind % 2, h, rows], d_recv.at[(r + 1) // rounds]
        return remote(part.at[r, k, h, rows], dst, ring_send, sem, target)

    def merge(n):
        r, k = n // chips, n % chips
        sib_o(n).wait_recv()
        sib_l(n).wait_recv()
        slot = n % 2
        (wa, wb), lse = weights(lown[slot], lrecv[n])
        for h in range(2):
            for i in range(blocks):
                cols = pl.ds((h * blocks + i) * lanes, lanes)
                part[r, k, h, block_rows(i)] = wa * own[slot, :, cols].astype(F32) + wb * orecv[n, :, cols].astype(F32)
            part[r, k, h, lse_row] = lse

        @pl.when(k == 0)
        def _():
            ring(r, 0).start()
            ring(r, 1).start()

        @pl.when(k == 1)
        def _():
            ring(r, 2).start()

        @pl.when(k == 3)
        def _():
            ring(r, 3).start()

    def relay(r):
        wait_bytes(frecv.at[r, :, rows], f_recv.at[r % 4])
        for kind in (4, 5):
            h = kind % 2
            k = (1, 3)[h]
            (wa, wb), lse = weights(part[r, k, h, lse_row], frecv[r, h, lse_row])
            for i in range(blocks):
                part[r, k, h, block_rows(i)] = wa * part[r, k, h, block_rows(i)] + wb * frecv[r, h, block_rows(i)]
            part[r, k, h, lse_row] = lse
            ring(r, kind).start()

    barrier = pltpu.get_barrier_semaphore()
    for neighbour in (left, right, sibling):
        pl.semaphore_signal(barrier, inc=1, device_id={'dcp': neighbour}, device_id_type=pl.DeviceIdType.MESH)
    for copy in q_load():
        copy.start()
    len_copy = pltpu.make_async_copy(len_hbm, len_ref, lensem)
    len_copy.start()
    for u in range(SLOTS - 1):
        fetch(u // 2, u % 2).start()
    pl.semaphore_wait(barrier, 3)
    for c in range(latent // lanes):
        to = pl.ds(c * group, group)
        for target in (right, left):
            remote(q_hbm.at[:, 0, :, c * lanes : (c + 1) * lanes], qbuf.at[0, me, to], ag_send, ag_recv.at[0, 0], target).start()
    wait_bytes(rope.at[:, 0], qsem.at[2])
    q_pack(0)
    to = pl.ds(latent_tiles, group // 2)
    for target in (right, left):
        remote(qbuf.at[0, me, to], qbuf.at[0, me, to], ag_send, ag_recv.at[0, 0], target).start()
    wait_bytes(qbuf.at[0, me, 0:latent_tiles], qsem.at[0])
    q_copy(0, 2, me, sibling).start()
    wait_bytes(rope.at[:, 1:], qsem.at[3])
    for r in range(1, rounds):
        q_pack(r)
    wait_bytes(qbuf.at[1:rounds, me, 0:latent_tiles], qsem.at[1])
    q_first(1)
    len_copy.wait()
    q_second(0)
    q_first(2)
    q_first(3)
    q_second(1)
    q_first(4)
    q_third(0)

    @pl.loop(0, rounds)
    def _(r):
        @pl.when(r + 2 < rounds)
        def _():
            q_second(r + 2)

        @pl.when(r + AHEAD + 2 < rounds)
        def _():
            q_first(r + AHEAD + 2)

        q_last(r)

        @pl.loop(0, chips)
        def _(k):
            n = r * chips + k

            @pl.when(jnp.logical_and(k == 2, r + 1 < rounds))
            def _():
                q_third(r + 1)

            o, lse = attend(n, 0)
            osend[n] = o
            lsend[n] = lse
            sib_o(n).start()
            sib_l(n).start()
            o, lse = attend(n, 1)
            own[n % 2] = o
            lown[n % 2] = lse

            @pl.when(n >= 1)
            def _():
                merge(n - 1)

        @pl.when(r >= 1)
        def _():
            relay(r - 1)

    merge(steps - 1)
    relay(rounds - 1)

    wait_bytes(drecv.at[0 : rounds - 1, :, :, rows], d_recv.at[0])

    @pl.loop(0, rounds - 1)
    def _(r):
        finish(part.at[r, 2], drecv.at[r], out_ref.at[r])

    wait_bytes(drecv.at[rounds - 1, :, :, rows], d_recv.at[1])

    wait_bytes(qbuf.at[:, 0:7], ag_send)
    wait_bytes(osend, sib_send.at[0])
    wait_bytes(lsend, sib_send.at[1])
    wait_bytes(part.at[:, 0:3, :, rows], ring_send)


def put_out(done, part, drecv, out_hbm, last, sems):
    n = done.shape[0]
    copies = [
        pltpu.make_async_copy(done, out_hbm.at[pl.ds(0, n)], sems.at[0]),
        pltpu.make_async_copy(last, out_hbm.at[n], sems.at[1]),
    ]
    copies[0].start()
    finish(part.at[n, 2], drecv.at[n], last)
    copies[1].start()
    for copy in copies:
        copy.wait()


def solution(mesh):
    group = mesh.shape['dcp']
    chips = group // CORES

    def local_step(q_blk, cache_blk, len_blk):
        batch, own_heads, width = q_blk.shape
        pages, page_len = cache_blk.shape[1], cache_blk.shape[3]
        latent = width - ROPE_DIM
        rounds = batch // group
        heads = own_heads * group
        steps = rounds * chips
        rows = latent // LANES // 2 * heads + 8
        q = q_blk.reshape(group, rounds, own_heads, width)
        cache = jnp.swapaxes(cache_blk, 3, 4).reshape(group, rounds, pages, 1, width, page_len)
        bf16 = jnp.bfloat16
        dma = pltpu.SemaphoreType.DMA
        tiles = group * latent // LANES + group // 2
        hbm = pl.BlockSpec(memory_space=pltpu.HBM)
        vmem = pl.BlockSpec(memory_space=pltpu.VMEM)
        done, part, drecv = pl.pallas_call(
            functools.partial(kernel, group),
            out_shape=[
                jax.ShapeDtypeStruct((rounds - 1, heads, latent), bf16),
                jax.ShapeDtypeStruct((rounds, chips, 2, rows, LANES), F32),
                jax.ShapeDtypeStruct((rounds, 2, 2, rows, LANES), F32),
            ],
            in_specs=[hbm, hbm, hbm],
            out_specs=[vmem] * 3,
            scratch_shapes=[
                pltpu.SMEM((batch,), jnp.int32),
                pltpu.VMEM((group, rounds, own_heads, ROPE_DIM), bf16),
                pltpu.VMEM((rounds, group, tiles, own_heads, LANES), bf16),
                pltpu.VMEM((SLOTS, pages, width, page_len), bf16),
                pltpu.VMEM((steps, heads, latent), bf16),
                pltpu.VMEM((steps, 1, heads), F32),
                pltpu.VMEM((steps, heads, latent), bf16),
                pltpu.VMEM((steps, 1, heads), F32),
                pltpu.VMEM((2, heads, latent), bf16),
                pltpu.VMEM((2, 1, heads), F32),
                pltpu.VMEM((rounds, 2, rows, LANES), F32),
                dma,
                dma((SLOTS,)),
                dma((4,)),
                dma,
                dma((REUSE, 2)),
                dma((REUSE,)),
                dma((2,)),
                dma((4, 2)),
                dma,
                dma((4,)),
                dma((2,)),
            ],
            compiler_params=pltpu.CompilerParams(
                collective_id=0, has_side_effects=True, vmem_limit_bytes=VMEM_BYTES),
        )(*(pltpu.with_memory_space_constraint(x, pltpu.HBM) for x in (len_blk, q, cache)))
        return pl.pallas_call(
            put_out,
            out_shape=jax.ShapeDtypeStruct((rounds, heads, latent), bf16),
            in_specs=[vmem] * 3,
            out_specs=hbm,
            scratch_shapes=[pltpu.VMEM((heads, latent), bf16), dma((2,))],
            compiler_params=pltpu.CompilerParams(vmem_limit_bytes=VMEM_BYTES),
        )(done, part, drecv)

    return jax.shard_map(
        local_step, mesh=mesh,
        in_specs=(P('dp', 'dcp', None), P('dp', None, 'dcp', None, None), P('dp')),
        out_specs=P(('dp', 'dcp'), None, None), check_vma=False)
```

```python
import functools

import jax
import jax.numpy as jnp
from jax import lax
from jax.experimental import pallas as pl
from jax.experimental.pallas import tpu as pltpu
from jax.sharding import PartitionSpec as P

ROPE_DIM = 64
QK_DIM = 192
CORES = 2
SLOTS = 3
AHEAD = 3
REUSE = 6
LANES = 128
VMEM_BYTES = 36 * 2**20
F32 = jnp.float32


def columns(row):
    return jnp.transpose(jnp.broadcast_to(row, (row.shape[1], row.shape[1])))


def weights(*lses):
    top = functools.reduce(jnp.maximum, lses)
    exps = [jnp.exp(one - top) for one in lses]
    total = functools.reduce(jnp.add, exps)
    return [columns(one / total) for one in exps], top + jnp.log(total)


def finish(local, received, out_ref):
    heads, latent = out_ref.shape
    blocks = latent // LANES // 2
    lse_row = pl.ds(blocks * heads, 1)
    for h in range(2):
        parts = [local.at[h], received.at[0, h], received.at[1, h]]
        cols, _ = weights(*(one[lse_row] for one in parts))
        for i in range(blocks):
            rows = pl.ds(i * heads, heads)
            total = functools.reduce(jnp.add, [col * one[rows] for col, one in zip(cols, parts)])
            out_ref[:, pl.ds((h * blocks + i) * LANES, LANES)] = total.astype(jnp.bfloat16)


def kernel(
    group, len_hbm, q_hbm, c_hbm, out_ref, part, drecv,
    len_ref, rope, qbuf, cbuf, osend, lsend, orecv, lrecv, own, lown, frecv,
    lensem, csem, qsem, ag_send, ag_recv, sib_q, sib_send, sib_recv, ring_send, f_recv, d_recv,
):
    rounds, _, tiles, own_heads, lanes = qbuf.shape
    chips = group // CORES
    steps = rounds * chips
    seqs = steps * CORES
    heads, latent = osend.shape[1:]
    blocks = latent // lanes // 2
    lse_row = pl.ds(blocks * heads, 1)
    rows = pl.ds(0, blocks * heads + 1)

    def block_rows(i):
        return pl.ds(i * heads, heads)
    pages, width, page_len = cbuf.shape[1:]
    me = lax.axis_index('dcp')
    chip, core = me // CORES, me % CORES
    sibling = chip * CORES + 1 - core
    right = ((chip + 1) % chips) * CORES + core
    left = ((chip + chips - 1) % chips) * CORES + core
    far = ((chip + 2) % chips) * CORES + core

    def remote(src, dst, send, recv, target):
        return pltpu.make_async_remote_copy(
            src_ref=src, dst_ref=dst, send_sem=send, recv_sem=recv,
            device_id={'dcp': target}, device_id_type=pl.DeviceIdType.MESH)

    def wait_bytes(ref, sem):
        pltpu.make_async_copy(ref, ref, sem).wait()

    def place(n, other):
        r, k = n // chips, n % chips
        dest_chip = (chip + 2 - k + chips) % chips
        dest_core = (1 - core) if other else core
        return r, dest_chip * CORES + dest_core

    def fetch(n, e):
        r, d = place(n, e == 0)
        slot = (2 * n + e) % SLOTS
        return pltpu.make_async_copy(c_hbm.at[d, r, :, 0], cbuf.at[slot], csem.at[slot])

    latent_tiles = group * latent // lanes

    def q_load():
        yield pltpu.make_async_copy(q_hbm.at[:, 0, :, latent:], rope.at[:, 0], qsem.at[2])
        for r in range(rounds):
            for c in range(latent // lanes):
                yield pltpu.make_async_copy(
                    q_hbm.at[:, r, :, c * lanes : (c + 1) * lanes], qbuf.at[r, me, c * group : (c + 1) * group],
                    qsem.at[min(r, 1)])
            if r == 0:
                yield pltpu.make_async_copy(q_hbm.at[:, 1:, :, latent:], rope.at[:, 1:], qsem.at[3])

    def q_pack(r):
        for p in range(group // 2):
            qbuf[r, me, latent_tiles + p] = jnp.concatenate([rope[2 * p, r], rope[2 * p + 1, r]], axis=1)

    def q_sem(r, kind):
        return sib_q.at[r % REUSE] if kind == 2 else ag_recv.at[r % REUSE, kind]

    def q_copy(r, kind, block, target):
        return remote(qbuf.at[r, block], qbuf.at[r, block], ag_send, q_sem(r, kind), target)

    def q_wait(r, kind, count):
        wait_bytes(qbuf.at[r, 0:count], q_sem(r, kind))

    def q_first(r):
        q_copy(r, 0, me, right).start()
        q_copy(r, 0, me, left).start()
        q_copy(r, 2, me, sibling).start()

    def q_second(r):
        q_wait(r, 0, 2)

        @pl.when(r % 2 == 0)
        def _():
            q_copy(r, 1, left, right).start()

        @pl.when(r % 2 == 1)
        def _():
            q_copy(r, 1, right, left).start()

        q_copy(r, 2, left, sibling).start()
        q_copy(r, 2, right, sibling).start()

    def q_third(r):
        q_wait(r, 1, 1)
        q_copy(r, 2, far, sibling).start()

    def q_last(r):
        q_wait(r, 2, chips)

    def attend(n, e):
        r, d = place(n, e == 0)
        slot = (2 * n + e) % SLOTS
        fetch(n, e).wait()
        nxt = 2 * n + e + SLOTS - 1

        @pl.when(nxt < seqs)
        def _():
            fetch((2 * n + e + SLOTS - 1) // 2, (e + SLOTS - 1) % 2).start()

        q = [qbuf[r, :, c * group + d].reshape(heads, lanes) for c in range(latent // lanes)]
        pair = qbuf[r, :, latent_tiles + d // 2].reshape(heads, lanes)
        q.append(jnp.where(d % 2 == 0, pair[:, : lanes // 2], pair[:, lanes // 2 :]))
        q = jnp.concatenate(q, axis=1)
        length = len_ref[d * rounds + r]
        scores = []
        for j in range(pages):
            s = jnp.dot(q, cbuf[slot, j], preferred_element_type=F32) * (QK_DIM ** -0.5)
            pos = lax.broadcasted_iota(jnp.int32, s.shape, 1) + (j * group + me) * page_len
            scores.append(jnp.where(pos < length, s, -1e30))
        top = functools.reduce(jnp.maximum, [jnp.max(s, axis=1, keepdims=True) for s in scores])
        exps = [jnp.exp(s - top) for s in scores]
        total = functools.reduce(jnp.add, [jnp.sum(w, axis=1, keepdims=True) for w in exps])
        acc = functools.reduce(jnp.add, [
            lax.dot_general(w.astype(jnp.bfloat16), cbuf[slot, j, :latent], (((1,), (1,)), ((), ())),
                            preferred_element_type=F32)
            for j, w in enumerate(exps)])
        lse = top + jnp.log(total)
        lse = jnp.transpose(jnp.broadcast_to(lse, (heads, heads)))[0:1]
        return (acc / total).astype(jnp.bfloat16), lse

    def sib_o(n):
        return remote(osend.at[n], orecv.at[n], sib_send.at[0], sib_recv.at[n % 4, 0], sibling)

    def sib_l(n):
        return remote(lsend.at[n], lrecv.at[n], sib_send.at[1], sib_recv.at[n % 4, 1], sibling)

    def ring(r, kind):
        target = right if kind % 2 == 0 else left
        k = (0, 0, 1, 3, 1, 3)[kind]
        h = (0, 1, 1, 0, 0, 1)[kind]
        if kind < 2:
            dst, sem = frecv.at[r, h, rows], f_recv.at[r % 4]
        else:
            dst, sem = drecv.at[r, kind % 2, h, rows], d_recv.at[(r + 1) // rounds]
        return remote(part.at[r, k, h, rows], dst, ring_send, sem, target)

    def merge(n):
        r, k = n // chips, n % chips
        sib_o(n).wait_recv()
        sib_l(n).wait_recv()
        slot = n % 2
        (wa, wb), lse = weights(lown[slot], lrecv[n])
        for h in range(2):
            for i in range(blocks):
                cols = pl.ds((h * blocks + i) * lanes, lanes)
                part[r, k, h, block_rows(i)] = wa * own[slot, :, cols].astype(F32) + wb * orecv[n, :, cols].astype(F32)
            part[r, k, h, lse_row] = lse

        @pl.when(k == 0)
        def _():
            ring(r, 0).start()
            ring(r, 1).start()

        @pl.when(k == 1)
        def _():
            ring(r, 2).start()

        @pl.when(k == 3)
        def _():
            ring(r, 3).start()

    def relay(r):
        wait_bytes(frecv.at[r, :, rows], f_recv.at[r % 4])
        for kind in (4, 5):
            h = kind % 2
            k = (1, 3)[h]
            (wa, wb), lse = weights(part[r, k, h, lse_row], frecv[r, h, lse_row])
            for i in range(blocks):
                part[r, k, h, block_rows(i)] = wa * part[r, k, h, block_rows(i)] + wb * frecv[r, h, block_rows(i)]
            part[r, k, h, lse_row] = lse
            ring(r, kind).start()

    barrier = pltpu.get_barrier_semaphore()
    for neighbour in (left, right, sibling):
        pl.semaphore_signal(barrier, inc=1, device_id={'dcp': neighbour}, device_id_type=pl.DeviceIdType.MESH)
    for copy in q_load():
        copy.start()
    len_copy = pltpu.make_async_copy(len_hbm, len_ref, lensem)
    len_copy.start()
    for u in range(SLOTS - 1):
        fetch(u // 2, u % 2).start()
    pl.semaphore_wait(barrier, 3)
    for c in range(latent // lanes):
        to = pl.ds(c * group, group)
        for target in (right, left):
            remote(q_hbm.at[:, 0, :, c * lanes : (c + 1) * lanes], qbuf.at[0, me, to], ag_send, ag_recv.at[0, 0], target).start()
    wait_bytes(rope.at[:, 0], qsem.at[2])
    q_pack(0)
    to = pl.ds(latent_tiles, group // 2)
    for target in (right, left):
        remote(qbuf.at[0, me, to], qbuf.at[0, me, to], ag_send, ag_recv.at[0, 0], target).start()
    wait_bytes(qbuf.at[0, me, 0:latent_tiles], qsem.at[0])
    q_copy(0, 2, me, sibling).start()
    wait_bytes(rope.at[:, 1:], qsem.at[3])
    for r in range(1, rounds):
        q_pack(r)
    wait_bytes(qbuf.at[1:rounds, me, 0:latent_tiles], qsem.at[1])
    q_first(1)
    len_copy.wait()
    q_second(0)
    q_first(2)
    q_first(3)
    q_second(1)
    q_first(4)
    q_third(0)

    @pl.loop(0, rounds)
    def _(r):
        @pl.when(r + 2 < rounds)
        def _():
            q_second(r + 2)

        @pl.when(r + AHEAD + 2 < rounds)
        def _():
            q_first(r + AHEAD + 2)

        q_last(r)

        @pl.loop(0, chips)
        def _(k):
            n = r * chips + k

            @pl.when(jnp.logical_and(k == 2, r + 1 < rounds))
            def _():
                q_third(r + 1)

            o, lse = attend(n, 0)
            osend[n] = o
            lsend[n] = lse
            sib_o(n).start()
            sib_l(n).start()
            o, lse = attend(n, 1)
            own[n % 2] = o
            lown[n % 2] = lse

            @pl.when(n >= 1)
            def _():
                merge(n - 1)

        @pl.when(r >= 1)
        def _():
            relay(r - 1)

    merge(steps - 1)
    relay(rounds - 1)

    wait_bytes(drecv.at[0 : rounds - 1, :, :, rows], d_recv.at[0])

    @pl.loop(0, rounds - 1)
    def _(r):
        finish(part.at[r, 2], drecv.at[r], out_ref.at[r])

    wait_bytes(qbuf.at[:, 0:7], ag_send)
    wait_bytes(osend, sib_send.at[0])
    wait_bytes(lsend, sib_send.at[1])
    wait_bytes(part.at[:, 0:3, :, rows], ring_send)
    wait_bytes(drecv.at[rounds - 1, :, :, rows], d_recv.at[1])


def put_out(done, part, drecv, out_hbm, last, sems):
    n = done.shape[0]
    copies = [
        pltpu.make_async_copy(done, out_hbm.at[pl.ds(0, n)], sems.at[0]),
        pltpu.make_async_copy(last, out_hbm.at[n], sems.at[1]),
    ]
    copies[0].start()
    finish(part.at[n, 2], drecv.at[n], last)
    copies[1].start()
    for copy in copies:
        copy.wait()


def solution(mesh):
    group = mesh.shape['dcp']
    chips = group // CORES

    def local_step(q_blk, cache_blk, len_blk):
        batch, own_heads, width = q_blk.shape
        pages, page_len = cache_blk.shape[1], cache_blk.shape[3]
        latent = width - ROPE_DIM
        rounds = batch // group
        heads = own_heads * group
        steps = rounds * chips
        rows = latent // LANES // 2 * heads + 8
        q = q_blk.reshape(group, rounds, own_heads, width)
        cache = jnp.swapaxes(cache_blk, 3, 4).reshape(group, rounds, pages, 1, width, page_len)
        bf16 = jnp.bfloat16
        dma = pltpu.SemaphoreType.DMA
        tiles = group * latent // LANES + group // 2
        hbm = pl.BlockSpec(memory_space=pltpu.HBM)
        vmem = pl.BlockSpec(memory_space=pltpu.VMEM)
        done, part, drecv = pl.pallas_call(
            functools.partial(kernel, group),
            out_shape=[
                jax.ShapeDtypeStruct((rounds - 1, heads, latent), bf16),
                jax.ShapeDtypeStruct((rounds, chips, 2, rows, LANES), F32),
                jax.ShapeDtypeStruct((rounds, 2, 2, rows, LANES), F32),
            ],
            in_specs=[hbm, hbm, hbm],
            out_specs=[vmem] * 3,
            scratch_shapes=[
                pltpu.SMEM((batch,), jnp.int32),
                pltpu.VMEM((group, rounds, own_heads, ROPE_DIM), bf16),
                pltpu.VMEM((rounds, group, tiles, own_heads, LANES), bf16),
                pltpu.VMEM((SLOTS, pages, width, page_len), bf16),
                pltpu.VMEM((steps, heads, latent), bf16),
                pltpu.VMEM((steps, 1, heads), F32),
                pltpu.VMEM((steps, heads, latent), bf16),
                pltpu.VMEM((steps, 1, heads), F32),
                pltpu.VMEM((2, heads, latent), bf16),
                pltpu.VMEM((2, 1, heads), F32),
                pltpu.VMEM((rounds, 2, rows, LANES), F32),
                dma,
                dma((SLOTS,)),
                dma((4,)),
                dma,
                dma((REUSE, 2)),
                dma((REUSE,)),
                dma((2,)),
                dma((4, 2)),
                dma,
                dma((4,)),
                dma((2,)),
            ],
            compiler_params=pltpu.CompilerParams(
                collective_id=0, has_side_effects=True, vmem_limit_bytes=VMEM_BYTES),
        )(*(pltpu.with_memory_space_constraint(x, pltpu.HBM) for x in (len_blk, q, cache)))
        return pl.pallas_call(
            put_out,
            out_shape=jax.ShapeDtypeStruct((rounds, heads, latent), bf16),
            in_specs=[vmem] * 3,
            out_specs=hbm,
            scratch_shapes=[pltpu.VMEM((heads, latent), bf16), dma((2,))],
            compiler_params=pltpu.CompilerParams(vmem_limit_bytes=VMEM_BYTES),
        )(done, part, drecv)

    return jax.shard_map(
        local_step, mesh=mesh,
        in_specs=(P('dp', 'dcp', None), P('dp', None, 'dcp', None, None), P('dp')),
        out_specs=P(('dp', 'dcp'), None, None), check_vma=False)
```

```python
import functools

import jax
import jax.numpy as jnp
from jax import lax
from jax.experimental import pallas as pl
from jax.experimental.pallas import tpu as pltpu
from jax.sharding import PartitionSpec as P

ROPE_DIM = 64
QK_DIM = 192
CORES = 2
SLOTS = 3
AHEAD = 3
REUSE = 6
LANES = 128
VMEM_BYTES = 36 * 2**20
F32 = jnp.float32


def columns(row):
    return jnp.transpose(jnp.broadcast_to(row, (row.shape[1], row.shape[1])))


def weights(*lses):
    top = functools.reduce(jnp.maximum, lses)
    exps = [jnp.exp(one - top) for one in lses]
    total = functools.reduce(jnp.add, exps)
    return [columns(one / total) for one in exps], top + jnp.log(total)


def finish(local, received, out_ref):
    heads, latent = out_ref.shape
    blocks = latent // LANES // 2
    lse_row = pl.ds(blocks * heads, 1)
    for h in range(2):
        parts = [local.at[h], received.at[0, h], received.at[1, h]]
        cols, _ = weights(*(one[lse_row] for one in parts))
        for i in range(blocks):
            rows = pl.ds(i * heads, heads)
            total = functools.reduce(jnp.add, [col * one[rows] for col, one in zip(cols, parts)])
            out_ref[:, pl.ds((h * blocks + i) * LANES, LANES)] = total.astype(jnp.bfloat16)


def kernel(
    group, len_hbm, q_hbm, c_hbm, out_ref, part, drecv,
    len_ref, rope, qbuf, cbuf, osend, lsend, orecv, lrecv, own, lown, frecv,
    csem, qsem, ag_send, ag_recv, sib_q, sib_send, sib_recv, ring_send, f_recv, d_recv,
):
    rounds, _, tiles, own_heads, lanes = qbuf.shape
    chips = group // CORES
    steps = rounds * chips
    seqs = steps * CORES
    heads, latent = osend.shape[1:]
    blocks = latent // lanes // 2
    lse_row = pl.ds(blocks * heads, 1)
    rows = pl.ds(0, blocks * heads + 1)

    def block_rows(i):
        return pl.ds(i * heads, heads)
    pages, width, page_len = cbuf.shape[1:]
    me = lax.axis_index('dcp')
    chip, core = me // CORES, me % CORES
    sibling = chip * CORES + 1 - core
    right = ((chip + 1) % chips) * CORES + core
    left = ((chip + chips - 1) % chips) * CORES + core
    far = ((chip + 2) % chips) * CORES + core

    def remote(src, dst, send, recv, target):
        return pltpu.make_async_remote_copy(
            src_ref=src, dst_ref=dst, send_sem=send, recv_sem=recv,
            device_id={'dcp': target}, device_id_type=pl.DeviceIdType.MESH)

    def wait_bytes(ref, sem):
        pltpu.make_async_copy(ref, ref, sem).wait()

    def place(n, other):
        r, k = n // chips, n % chips
        dest_chip = (chip + 2 - k + chips) % chips
        dest_core = (1 - core) if other else core
        return r, dest_chip * CORES + dest_core

    def fetch(n, e):
        r, d = place(n, e == 0)
        slot = (2 * n + e) % SLOTS
        return pltpu.make_async_copy(c_hbm.at[d, r, :, 0], cbuf.at[slot], csem.at[slot])

    latent_tiles = group * latent // lanes

    def q_load():
        yield pltpu.make_async_copy(q_hbm.at[:, 0, :, latent:], rope.at[:, 0], qsem.at[2])
        for r in range(rounds):
            for c in range(latent // lanes):
                yield pltpu.make_async_copy(
                    q_hbm.at[:, r, :, c * lanes : (c + 1) * lanes], qbuf.at[r, me, c * group : (c + 1) * group],
                    qsem.at[min(r, 1)])
            if r == 0:
                yield pltpu.make_async_copy(q_hbm.at[:, 1:, :, latent:], rope.at[:, 1:], qsem.at[3])

    def q_pack(r):
        for p in range(group // 2):
            qbuf[r, me, latent_tiles + p] = jnp.concatenate([rope[2 * p, r], rope[2 * p + 1, r]], axis=1)

    def q_sem(r, kind):
        return sib_q.at[r % REUSE] if kind == 2 else ag_recv.at[r % REUSE, kind]

    def q_copy(r, kind, block, target):
        return remote(qbuf.at[r, block], qbuf.at[r, block], ag_send, q_sem(r, kind), target)

    def q_wait(r, kind, count):
        wait_bytes(qbuf.at[r, 0:count], q_sem(r, kind))

    def q_first(r):
        q_copy(r, 0, me, right).start()
        q_copy(r, 0, me, left).start()
        q_copy(r, 2, me, sibling).start()

    def q_second(r):
        q_wait(r, 0, 2)

        @pl.when(r % 2 == 0)
        def _():
            q_copy(r, 1, left, right).start()

        @pl.when(r % 2 == 1)
        def _():
            q_copy(r, 1, right, left).start()

        q_copy(r, 2, left, sibling).start()
        q_copy(r, 2, right, sibling).start()

    def q_third(r):
        q_wait(r, 1, 1)
        q_copy(r, 2, far, sibling).start()

    def q_last(r):
        q_wait(r, 2, chips)

    def attend(n, e):
        r, d = place(n, e == 0)
        slot = (2 * n + e) % SLOTS
        fetch(n, e).wait()
        nxt = 2 * n + e + SLOTS - 1

        @pl.when(nxt < seqs)
        def _():
            fetch((2 * n + e + SLOTS - 1) // 2, (e + SLOTS - 1) % 2).start()

        q = [qbuf[r, :, c * group + d].reshape(heads, lanes) for c in range(latent // lanes)]
        pair = qbuf[r, :, latent_tiles + d // 2].reshape(heads, lanes)
        q.append(jnp.where(d % 2 == 0, pair[:, : lanes // 2], pair[:, lanes // 2 :]))
        q = jnp.concatenate(q, axis=1)
        length = len_ref[d * rounds + r]
        scores = []
        for j in range(pages):
            s = jnp.dot(q, cbuf[slot, j], preferred_element_type=F32) * (QK_DIM ** -0.5)
            pos = lax.broadcasted_iota(jnp.int32, s.shape, 1) + (j * group + me) * page_len
            scores.append(jnp.where(pos < length, s, -1e30))
        top = functools.reduce(jnp.maximum, [jnp.max(s, axis=1, keepdims=True) for s in scores])
        exps = [jnp.exp(s - top) for s in scores]
        total = functools.reduce(jnp.add, [jnp.sum(w, axis=1, keepdims=True) for w in exps])
        acc = functools.reduce(jnp.add, [
            lax.dot_general(w.astype(jnp.bfloat16), cbuf[slot, j, :latent], (((1,), (1,)), ((), ())),
                            preferred_element_type=F32)
            for j, w in enumerate(exps)])
        lse = top + jnp.log(total)
        lse = jnp.transpose(jnp.broadcast_to(lse, (heads, heads)))[0:1]
        return (acc / total).astype(jnp.bfloat16), lse

    def sib_o(n):
        return remote(osend.at[n], orecv.at[n], sib_send.at[0], sib_recv.at[n % 4, 0], sibling)

    def sib_l(n):
        return remote(lsend.at[n], lrecv.at[n], sib_send.at[1], sib_recv.at[n % 4, 1], sibling)

    def ring(r, kind):
        target = right if kind % 2 == 0 else left
        k = (0, 0, 1, 3, 1, 3)[kind]
        h = (0, 1, 1, 0, 0, 1)[kind]
        if kind < 2:
            dst, sem = frecv.at[r, h, rows], f_recv.at[r % 4]
        else:
            dst, sem = drecv.at[r, kind % 2, h, rows], d_recv.at[(r + 1) // rounds]
        return remote(part.at[r, k, h, rows], dst, ring_send, sem, target)

    def merge(n):
        r, k = n // chips, n % chips
        sib_o(n).wait_recv()
        sib_l(n).wait_recv()
        slot = n % 2
        (wa, wb), lse = weights(lown[slot], lrecv[n])
        for h in range(2):
            for i in range(blocks):
                cols = pl.ds((h * blocks + i) * lanes, lanes)
                part[r, k, h, block_rows(i)] = wa * own[slot, :, cols].astype(F32) + wb * orecv[n, :, cols].astype(F32)
            part[r, k, h, lse_row] = lse

        @pl.when(k == 0)
        def _():
            ring(r, 0).start()
            ring(r, 1).start()

        @pl.when(k == 1)
        def _():
            ring(r, 2).start()

        @pl.when(k == 3)
        def _():
            ring(r, 3).start()

    def relay(r):
        wait_bytes(frecv.at[r, :, rows], f_recv.at[r % 4])
        for kind in (4, 5):
            h = kind % 2
            k = (1, 3)[h]
            (wa, wb), lse = weights(part[r, k, h, lse_row], frecv[r, h, lse_row])
            for i in range(blocks):
                part[r, k, h, block_rows(i)] = wa * part[r, k, h, block_rows(i)] + wb * frecv[r, h, block_rows(i)]
            part[r, k, h, lse_row] = lse
            ring(r, kind).start()

    barrier = pltpu.get_barrier_semaphore()
    for neighbour in (left, right, sibling):
        pl.semaphore_signal(barrier, inc=1, device_id={'dcp': neighbour}, device_id_type=pl.DeviceIdType.MESH)
    for copy in q_load():
        copy.start()
    for u in range(SLOTS - 1):
        fetch(u // 2, u % 2).start()
    pl.semaphore_wait(barrier, 3)
    for c in range(latent // lanes):
        to = pl.ds(c * group, group)
        for target in (right, left):
            remote(q_hbm.at[:, 0, :, c * lanes : (c + 1) * lanes], qbuf.at[0, me, to], ag_send, ag_recv.at[0, 0], target).start()
    wait_bytes(rope.at[:, 0], qsem.at[2])
    q_pack(0)
    to = pl.ds(latent_tiles, group // 2)
    for target in (right, left):
        remote(qbuf.at[0, me, to], qbuf.at[0, me, to], ag_send, ag_recv.at[0, 0], target).start()
    wait_bytes(qbuf.at[0, me, 0:latent_tiles], qsem.at[0])
    len_copy = pltpu.make_async_copy(len_hbm, len_ref, qsem.at[0])
    len_copy.start()
    q_copy(0, 2, me, sibling).start()
    wait_bytes(rope.at[:, 1:], qsem.at[3])
    for r in range(1, rounds):
        q_pack(r)
    wait_bytes(qbuf.at[1:rounds, me, 0:latent_tiles], qsem.at[1])
    q_first(1)
    len_copy.wait()
    q_second(0)
    q_first(2)
    q_first(3)
    q_second(1)
    q_first(4)
    q_third(0)

    @pl.loop(0, rounds)
    def _(r):
        @pl.when(r + 2 < rounds)
        def _():
            q_second(r + 2)

        @pl.when(r + AHEAD + 2 < rounds)
        def _():
            q_first(r + AHEAD + 2)

        q_last(r)

        @pl.loop(0, chips)
        def _(k):
            n = r * chips + k

            @pl.when(jnp.logical_and(k == 2, r + 1 < rounds))
            def _():
                q_third(r + 1)

            o, lse = attend(n, 0)
            osend[n] = o
            lsend[n] = lse
            sib_o(n).start()
            sib_l(n).start()
            o, lse = attend(n, 1)
            own[n % 2] = o
            lown[n % 2] = lse

            @pl.when(n >= 1)
            def _():
                merge(n - 1)

        @pl.when(r >= 1)
        def _():
            relay(r - 1)

    merge(steps - 1)
    relay(rounds - 1)

    wait_bytes(drecv.at[0 : rounds - 1, :, :, rows], d_recv.at[0])

    @pl.loop(0, rounds - 1)
    def _(r):
        finish(part.at[r, 2], drecv.at[r], out_ref.at[r])

    wait_bytes(qbuf.at[:, 0:7], ag_send)
    wait_bytes(osend, sib_send.at[0])
    wait_bytes(lsend, sib_send.at[1])
    wait_bytes(part.at[:, 0:3, :, rows], ring_send)
    wait_bytes(drecv.at[rounds - 1, :, :, rows], d_recv.at[1])


def put_out(done, part, drecv, out_hbm, last, sems):
    n = done.shape[0]
    copies = [
        pltpu.make_async_copy(done, out_hbm.at[pl.ds(0, n)], sems.at[0]),
        pltpu.make_async_copy(last, out_hbm.at[n], sems.at[1]),
    ]
    copies[0].start()
    finish(part.at[n, 2], drecv.at[n], last)
    copies[1].start()
    for copy in copies:
        copy.wait()


def solution(mesh):
    group = mesh.shape['dcp']
    chips = group // CORES

    def local_step(q_blk, cache_blk, len_blk):
        batch, own_heads, width = q_blk.shape
        pages, page_len = cache_blk.shape[1], cache_blk.shape[3]
        latent = width - ROPE_DIM
        rounds = batch // group
        heads = own_heads * group
        steps = rounds * chips
        rows = latent // LANES // 2 * heads + 8
        q = q_blk.reshape(group, rounds, own_heads, width)
        cache = jnp.swapaxes(cache_blk, 3, 4).reshape(group, rounds, pages, 1, width, page_len)
        bf16 = jnp.bfloat16
        dma = pltpu.SemaphoreType.DMA
        tiles = group * latent // LANES + group // 2
        hbm = pl.BlockSpec(memory_space=pltpu.HBM)
        vmem = pl.BlockSpec(memory_space=pltpu.VMEM)
        done, part, drecv = pl.pallas_call(
            functools.partial(kernel, group),
            out_shape=[
                jax.ShapeDtypeStruct((rounds - 1, heads, latent), bf16),
                jax.ShapeDtypeStruct((rounds, chips, 2, rows, LANES), F32),
                jax.ShapeDtypeStruct((rounds, 2, 2, rows, LANES), F32),
            ],
            in_specs=[hbm, hbm, hbm],
            out_specs=[vmem] * 3,
            scratch_shapes=[
                pltpu.SMEM((batch,), jnp.int32),
                pltpu.VMEM((group, rounds, own_heads, ROPE_DIM), bf16),
                pltpu.VMEM((rounds, group, tiles, own_heads, LANES), bf16),
                pltpu.VMEM((SLOTS, pages, width, page_len), bf16),
                pltpu.VMEM((steps, heads, latent), bf16),
                pltpu.VMEM((steps, 1, heads), F32),
                pltpu.VMEM((steps, heads, latent), bf16),
                pltpu.VMEM((steps, 1, heads), F32),
                pltpu.VMEM((2, heads, latent), bf16),
                pltpu.VMEM((2, 1, heads), F32),
                pltpu.VMEM((rounds, 2, rows, LANES), F32),
                dma((SLOTS,)),
                dma((4,)),
                dma,
                dma((REUSE, 2)),
                dma((REUSE,)),
                dma((2,)),
                dma((4, 2)),
                dma,
                dma((4,)),
                dma((2,)),
            ],
            compiler_params=pltpu.CompilerParams(
                collective_id=0, has_side_effects=True, vmem_limit_bytes=VMEM_BYTES),
        )(*(pltpu.with_memory_space_constraint(x, pltpu.HBM) for x in (len_blk, q, cache)))
        return pl.pallas_call(
            put_out,
            out_shape=jax.ShapeDtypeStruct((rounds, heads, latent), bf16),
            in_specs=[vmem] * 3,
            out_specs=hbm,
            scratch_shapes=[pltpu.VMEM((heads, latent), bf16), dma((2,))],
            compiler_params=pltpu.CompilerParams(vmem_limit_bytes=VMEM_BYTES),
        )(done, part, drecv)

    return jax.shard_map(
        local_step, mesh=mesh,
        in_specs=(P('dp', 'dcp', None), P('dp', None, 'dcp', None, None), P('dp')),
        out_specs=P(('dp', 'dcp'), None, None), check_vma=False)
```
